256 devices in a mesh: dp: 16 (over z, x_lo), rep: 4 (over y), ind: 4 (over x_hi, core).
Axes of the slice: x: 4 (x_hi: 2, x_lo: 2; x = x_hi * 2 + x_lo), y: 4, z: 8, core: 2. Of those that a mesh axis runs over, the one named last changes fastest.
Arguments:
- points: bfloat16 [49152, 64], P(('dp', 'rep')), may hold values from -6 to 6
- targets: float32 [49152], P(('dp', 'rep')), may hold values from -6 to 6
- inducing: float32 [4096, 64], P('ind'), may hold values from -6 to 6
- whitening: bfloat16 [4096, 4096], P('ind'), may hold values from -0.01953125 to 0.01953125
- mean_v: float32 [4096], P('ind'), may hold values from -12 to 12
- covariance: float32 [4096, 4096], P('ind', ('dp', 'rep')), may hold values from -24 to 24
- precision: float32 [4096, 4096], P('ind', ('dp', 'rep')), may hold values from -3 to 3
- natural_one: float32 [4096], P('ind'), may hold values from -6 to 6
- lengthscales: float32 [64], replicated, may hold values from 1.6 to 24
- hypers: float32 [2], replicated, may hold values from 0.5 to 2
Outputs:
- precision_new: float32 [4096, 4096], P('ind', ('dp', 'rep'))
- natural_new: float32 [4096], P('ind')
- expected_fit: float32 [], replicated
The draws below stay inside these ranges and needn't reach their ends.
All inputs are finite; a program needn't handle non-finite values.
Results may differ from the reference program's by a relative error of at most 0.0076.
Values may be sent and summed in bfloat16 or wider, within the bound.
A program may use at most 128 MiB of HBM per device.

```python
import math
import jax
import jax.numpy as jnp
from jax import lax

M = 4096
F = 64
TOK_DEV = 768
TOKENS = 49152


def block_scale(stream_key, extent, split, least, largest):
    level = 1.0
    for axis_at, parts in split:
        steps = jax.random.uniform(jax.random.fold_in(jax.random.fold_in(stream_key, 6), axis_at), (parts,), jnp.float32, least / len(split), largest / len(split))
        level = level * jnp.repeat(jnp.exp(steps), extent[axis_at] // parts).reshape((-1,) + (1,) * (len(extent) - 1 - axis_at))
    return level


def scatter_about(own_key, extent, scale, most, shards=(), held_as=jnp.bfloat16):
    values = scale * jax.random.normal(own_key, extent, jnp.float32)
    if shards:
        values = values * block_scale(own_key, extent, shards, -0.22, 0.18)
    return jnp.clip(values, -most, most).astype(held_as)


def setup_inputs(seed: int = 0) -> dict:
    seeds = jax.random.split(jax.random.key(seed), 11)
    return {
        "points": scatter_about(seeds[0], (TOKENS, F), 1.0, 6.0, ((0, 64),)),
        "targets": scatter_about(seeds[1], (TOKENS,), 1.0, 6.0, ((0, 64),), jnp.float32),
        "inducing": scatter_about(seeds[2], (M, F), 1.0, 6.0, ((0, 4),), jnp.float32),
        "whitening": scatter_about(seeds[3], (M, M), (TOKENS * M // 2048) ** -0.5, 0.01953125, ((0, 4),)),
        "mean_v": scatter_about(seeds[4], (M,), 2.0, 12.0, ((0, 4),), jnp.float32),
        "covariance": scatter_about(seeds[5], (M, M), 4.0, 24.0, ((0, 4), (1, 64)), jnp.float32),
        "precision": scatter_about(seeds[6], (M, M), 0.5, 3.0, ((0, 4), (1, 64)), jnp.float32),
        "natural_one": scatter_about(seeds[7], (M,), 1.0, 6.0, ((0, 4),), jnp.float32),
        "lengthscales": jnp.clip(jnp.exp(jax.random.uniform(seeds[8], (F,), jnp.float32, math.log(1.6), math.log(24.0))), 1.6, 24.0),
        "hypers": jnp.clip(jnp.exp(jax.random.uniform(seeds[9], (2,), jnp.float32, math.log(0.5), math.log(2.0))), 0.5, 2.0),
    }


def cross_cov(inducing, points, lengthscales, signal):
    scaled_z = inducing / lengthscales
    scaled_x = points.astype(jnp.float32) / lengthscales
    norm_z = jnp.sum(scaled_z * scaled_z, axis=1)
    norm_x = jnp.sum(scaled_x * scaled_x, axis=1)
    inner = jnp.dot(scaled_z, scaled_x.T, precision=lax.Precision.HIGHEST)
    return (signal * jnp.exp(-0.5 * (norm_z[:, None] + norm_x[None, :] - 2.0 * inner))).astype(jnp.bfloat16)


def reference(points, targets, inducing, whitening, mean_v, covariance, precision, natural_one, lengthscales, hypers):
    signal = hypers[0]
    noise_var = hypers[1]
    total = points.shape[0]
    blocks = total // TOK_DEV
    point_blocks = points.reshape(blocks, TOK_DEV, F)
    target_blocks = targets.reshape(blocks, TOK_DEV)

    def accumulate(carry, pieces):
        gram, proj, fit_sum = carry
        block_pts, block_tgt = pieces
        cross = cross_cov(inducing, block_pts, lengthscales, signal)
        white = jnp.dot(whitening, cross, preferred_element_type=jnp.float32).astype(jnp.bfloat16)
        white_wide = white.astype(jnp.float32)
        pred_mean = jnp.dot(mean_v, white_wide, precision=lax.Precision.HIGHEST)
        sq_norm = jnp.sum(white_wide * white_wide, axis=0)
        resid = block_tgt - pred_mean
        fit_sum = fit_sum + jnp.sum(resid * resid + signal - sq_norm)
        proj = proj + jnp.dot(white_wide, block_tgt, precision=lax.Precision.HIGHEST)
        gram = gram + lax.dot_general(white, white, (((1,), (1,)), ((), ())), preferred_element_type=jnp.float32)
        return (gram, proj, fit_sum), None

    start = (jnp.zeros((M, M), jnp.float32), jnp.zeros((M,), jnp.float32), jnp.zeros((), jnp.float32))
    (gram, proj, fit_sum), unused = lax.scan(accumulate, start, (point_blocks, target_blocks))
    trace = jnp.sum(covariance * gram)
    expected_fit = -0.5 * jnp.log(2.0 * jnp.pi * noise_var) - (fit_sum + trace) / (2.0 * noise_var * total)
    precision_new = 0.5 * precision + 0.5 * (jnp.eye(M, dtype=jnp.float32) + gram / noise_var)
    natural_new = 0.5 * natural_one + 0.5 * proj / noise_var
    return precision_new, natural_new, expected_fit
```

```python
import jax
import jax.numpy as jnp
from jax import lax
from jax.experimental import pallas as pl
from jax.experimental.pallas import tpu as pltpu
from jax.sharding import Mesh
from jax.sharding import PartitionSpec as P

AXES = ("dp_0", "dp_1", "rep", "ind_0", "ind_1")
IND = ("ind_0", "ind_1")
DP_REP = ("dp_0", "dp_1", "rep")
MESH = pl.DeviceIdType.MESH
VMEM = pl.BlockSpec(memory_space=pltpu.VMEM)
ANY = pl.BlockSpec(memory_space=pl.ANY)
F32 = jnp.float32
BF16 = jnp.bfloat16
ROUNDS = 10


def place():
    return tuple(lax.axis_index(a) for a in AXES)


def remote(src, dst, send, recv, to):
    return pltpu.make_async_remote_copy(
        src_ref=src, dst_ref=dst, send_sem=send, recv_sem=recv, device_id=to, device_id_type=MESH
    )


def share_kernel(z_ref, p_ref, t_ref, allz, p_out, t_out, send, recv, local):
    z, lo, y, hi, core = place()
    mine = hi * 2 + core
    other = (1 - hi) * 2 + core
    partner = (z, lo, y, hi, 1 - core)
    across = (z, 1 - lo, y, 1 - hi, core)
    swap = (z, 1 - lo, y, hi, core)
    over = remote(z_ref, allz.at[mine], send.at[0], recv.at[0], across)
    over.start()

    @pl.when(hi == 0)
    def _():
        remote(p_ref, p_out, send.at[3], recv.at[3], swap).start()
        remote(t_ref, t_out, send.at[4], recv.at[4], swap).start()

    near = remote(z_ref, allz.at[mine], send.at[1], recv.at[1], partner)
    near.start()
    own = pltpu.make_async_copy(z_ref, allz.at[mine], local)
    own.start()

    @pl.when(hi == 1)
    def _():
        p_out[...] = p_ref[...]
        t_out[...] = t_ref[...]

    over.wait_recv()
    on = remote(allz.at[other], allz.at[other], send.at[2], recv.at[2], partner)
    on.start()
    own.wait()
    near.wait_recv()
    on.wait_recv()

    @pl.when(hi == 0)
    def _():
        remote(p_ref, p_out, send.at[3], recv.at[3], swap).wait()
        remote(t_ref, t_out, send.at[4], recv.at[4], swap).wait()

    over.wait_send()
    near.wait_send()
    on.wait_send()


def share(z_t, p_t, tgt):
    return pl.pallas_call(
        share_kernel,
        out_shape=(
            jax.ShapeDtypeStruct((4, *z_t.shape), F32),
            jax.ShapeDtypeStruct(p_t.shape, BF16),
            jax.ShapeDtypeStruct(tgt.shape, F32),
        ),
        in_specs=[VMEM] * 3,
        out_specs=(VMEM, VMEM, VMEM),
        scratch_shapes=[
            pltpu.SemaphoreType.DMA((5,)),
            pltpu.SemaphoreType.DMA((5,)),
            pltpu.SemaphoreType.DMA,
        ],
        compiler_params=pltpu.CompilerParams(has_side_effects=True),
        name="share",
    )(z_t, p_t, tgt)


def round_of(t):
    late = jnp.minimum(t // 2, 1)
    is_b = (t % 2) * late
    a = t * (1 - late) + (1 + t // 2) * late
    is_h = (1 - is_b) * (a // 4)
    g = is_b * (t // 2 - 1) + (1 - is_b) * (a - 4 * is_h)
    return is_b, is_h, g


def gram_kernel(
    white, pm_ref, out, pm_out,
    wbuf, pay, y1, y2, zs, zr, xk, xs, xr, fin, fint, own, pmr,
    g_s, g_r, p_s, p_r, y1_s, y1_r, y2_s, y2_r, z_s, z_r, x_s, x_r, pm_s, pm_r, f_s, own_sem, w_sem,
):
    z, lo, y, hi, core = place()
    mine = hi * 2 + core
    yp, ym, y2p = (y + 1) % 4, (y + 3) % 4, (y + 2) % 4
    partner = (z, lo, y, hi, 1 - core)
    gather_to = (z, 1 - lo, y, 1 - hi, (core + 1 - hi) % 2)

    load = pltpu.make_async_copy(white, wbuf.at[core], w_sem)
    load.start()
    pm_to = (partner, (z, 1 - lo, y, 1 - hi, core), (z, 1 - lo, y, 1 - hi, 1 - core))
    pm_copies = [remote(pm_ref, pmr.at[k], pm_s.at[k], pm_r.at[k], to) for k, to in enumerate(pm_to)]
    for c in pm_copies:
        c.start()
    load.wait()

    def gather_piece(g, k):
        rows = pl.ds(pl.multiple_of(k * 128 + 32 * g, 32), 32)
        return remote(wbuf.at[core, rows], wbuf.at[2, rows], g_s.at[g], g_r.at[g], gather_to)

    def gather_start(g, _):
        lax.fori_loop(0, 8, lambda k, c: (gather_piece(g, k).start(), c)[1], 0)
        return 0

    lax.fori_loop(0, 4, gather_start, 0)
    to_partner = remote(wbuf.at[core], wbuf.at[core], p_s, p_r, partner)
    to_partner.start()

    def gather_all(g):
        rows = pl.ds(0, 256)
        return remote(wbuf.at[core, rows], wbuf.at[2, rows], g_s.at[g], g_r.at[g], gather_to)

    def y1_copies(t):
        up = pl.ds(pl.multiple_of(y2p * 64, 64), 32)
        down = pl.ds(pl.multiple_of(y2p * 64 + 32, 32), 32)
        return (
            remote(pay.at[t, up], y1.at[t, 0], y1_s.at[t, 0], y1_r.at[t, 0], (z, lo, yp, hi, core)),
            remote(pay.at[t, down], y1.at[t, 1], y1_s.at[t, 1], y1_r.at[t, 1], (z, lo, ym, hi, core)),
        )

    def y2_copies(t):
        up = pl.ds(pl.multiple_of(yp * 64, 64), 64)
        down = pl.ds(pl.multiple_of(ym * 64, 64), 64)
        return (
            remote(pay.at[t, up], y2.at[t, 0], y2_s.at[t, 0], y2_r.at[t, 0], (z, lo, yp, hi, core)),
            remote(pay.at[t, down], y2.at[t, 1], y2_s.at[t, 1], y2_r.at[t, 1], (z, lo, ym, hi, core)),
        )

    def z_copy(t, d):
        to = (z + d) % 8
        cols = pl.ds(pl.multiple_of(to * 128, 128), 128)
        return remote(zs.at[t, :, cols], zr.at[t, d - 1], z_s.at[t], z_r.at[t], (to, lo, y, hi, core))

    def z_all(t):
        return remote(zr.at[t], zr.at[t], z_s.at[t], z_r.at[t], ((z + 1) % 8, lo, y, hi, core))

    def x_copy(t):
        return remote(xs.at[t], xr.at[t], x_s.at[t], x_r.at[t], (z, 1 - lo, y, hi, core))

    def compute(t):
        is_b, is_h, g = round_of(t)
        plain = 1 - is_h

        @pl.when(is_b == 1)
        def _():
            gather_all(g).wait_recv()

        @pl.when(is_h * (1 - g) == 1)
        def _():
            to_partner.wait_recv()

        left = is_b * 2 + is_h + plain * (1 - is_b) * core
        right = plain * core
        shift = g + is_h * 2 * core
        a = jnp.concatenate(
            [wbuf[left, pl.ds(pl.multiple_of(k * 128 + 32 * shift, 32), 32), :] for k in range(8)], axis=0
        )
        for j in range(4):
            b = wbuf[right, j * 256 : (j + 1) * 256, :]
            part = lax.dot_general(a, b, (((1,), (1,)), ((), ())), preferred_element_type=F32)
            pay[t, :, j * 256 : (j + 1) * 256] = part.astype(BF16)
        for c in y1_copies(t):
            c.start()

    def after_y1(t):
        for k, c in enumerate(y1_copies(t)):
            c.wait_recv()
            rows = pl.ds(pl.multiple_of((yp, ym)[k] * 64 + 32 * k, 32), 32)
            pay[t, rows, :] = (pay[t, rows, :].astype(F32) + y1[t, k].astype(F32)).astype(BF16)
        for c in y2_copies(t):
            c.start()

    def after_y2(t):
        for c in y2_copies(t):
            c.wait_recv()
        rows = pl.ds(pl.multiple_of(y * 64, 64), 64)
        total = pay[t, rows, :].astype(F32) + y2[t, 0].astype(F32) + y2[t, 1].astype(F32)
        zs[t] = total.astype(BF16)
        for d in range(1, 8):
            z_copy(t, d).start()

    def after_z(t):
        z_all(t).wait_recv()
        total = zs[t, :, pl.ds(pl.multiple_of(z * 128, 128), 128)].astype(F32)
        for d in range(7):
            total = total + zr[t, d].astype(F32)
        xk[t] = total

        xs[t] = xk[t, pl.ds(pl.multiple_of((1 - lo) * 32, 32), 32), :].astype(BF16)
        x_copy(t).start()

    def after_x(t):
        x_copy(t).wait_recv()
        is_b, is_h, g = round_of(t)
        total = xk[t, pl.ds(pl.multiple_of(lo * 32, 32), 32), :] + xr[t].astype(F32)
        slot = is_b + 2 * is_h
        row = g * 32 + is_h * core * 64
        fin[slot, pl.ds(pl.multiple_of(row, 32), 32), :] = total.astype(BF16)

    zero = jnp.zeros((128, 128), BF16)
    fin[2] = zero

    def step(t, carry):
        for lag, work in ((4, after_x), (3, after_z), (2, after_y2), (1, after_y1), (0, compute)):

            @pl.when((t >= lag) & (t < ROUNDS + lag))
            def _(lag=lag, work=work):
                work(t - lag)

        return carry

    lax.fori_loop(0, ROUNDS + 4, step, 0)

    fint[0] = fin[1].astype(F32).T.astype(BF16)
    fint[1] = fin[2].astype(F32).T.astype(BF16)

    nxt = (1 - hi) * 2 + (core + hi) % 2
    low, high = hi * 2, hi * 2 + 1
    me = (((z * 2 + lo) * 4 + y) * 2 + hi) * 2 + core
    direct = pl.ds(pl.multiple_of(z * 128, 128), 128)
    mirror = pl.ds(pl.multiple_of(256 * y + 128 * lo, 128), 128)

    def owner(q, ind):
        return (q // 8, (q // 4) % 2, q % 4, ind // 2, ind % 2)

    sends = []
    for e in range(2):
        rows = slice(64 * e, 64 * e + 64)
        sends.append((fin.at[0, rows], own.at[0, :, direct], own_sem.at[0], owner(16 * mine + 4 * y + 2 * lo + e, mine)))
        sends.append((fin.at[1, rows], own.at[0, :, direct], own_sem.at[0], owner(16 * nxt + 4 * y + 2 * lo + e, mine)))
        sends.append((fint.at[0, rows], own.at[0, :, mirror], own_sem.at[0], owner(16 * mine + 2 * z + e, nxt)))
        sends.append((fint.at[1, rows], own.at[core, :, mirror], own_sem.at[core], owner(16 * low + 2 * z + e, high)))
    half = pl.ds(pl.multiple_of(64 * core, 64), 64)
    sends.append((fin.at[2, half], own.at[0, :, direct], own_sem.at[0], owner(16 * high + 4 * y + 2 * lo + core, low)))

    def flat(d):
        return (((d[0] * 2 + d[1]) * 4 + d[2]) * 2 + d[3]) * 2 + d[4]

    for k, (src, dst, sem, to) in enumerate(sends):

        @pl.when(flat(to) != me)
        def _(k=k, src=src, dst=dst, sem=sem, to=to):
            remote(src, dst, f_s.at[k], sem, to).start()

        @pl.when(flat(to) == me)
        def _(src=src, dst=dst, sem=sem):
            pltpu.make_async_copy(src, dst, sem).start()

    for c in pm_copies:
        c.wait_recv()
    pm_out[...] = pm_ref[...] + pmr[0] + pmr[1] + pmr[2]

    pltpu.make_async_copy(own.at[0], own.at[0], own_sem.at[0]).wait()
    both = core * (1 - jnp.minimum(jnp.abs(z // 2 - low), 1))

    @pl.when(both == 0)
    def _():
        out[...] = own[0]

    @pl.when(both == 1)
    def _():
        pltpu.make_async_copy(own.at[1], own.at[1], own_sem.at[1]).wait()
        out[...] = own[0] + own[1]

    for k, (src, dst, sem, to) in enumerate(sends):

        @pl.when(flat(to) != me)
        def _(k=k, src=src, dst=dst, sem=sem, to=to):
            remote(src, dst, f_s.at[k], sem, to).wait_send()

    for c in pm_copies:
        c.wait_send()
    to_partner.wait_send()

    def drain(t, carry):
        for c in y1_copies(t) + y2_copies(t):
            c.wait_send()
        z_all(t).wait_send()
        x_copy(t).wait_send()
        return carry

    lax.fori_loop(0, ROUNDS, drain, 0)
    lax.fori_loop(0, 4, lambda g, c: (gather_all(g).wait_send(), c)[1], 0)


def gram_reduced(white, pm):
    dma = pltpu.SemaphoreType.DMA
    n = white.shape[1]
    return pl.pallas_call(
        gram_kernel,
        out_shape=(jax.ShapeDtypeStruct((64, 1024), BF16), jax.ShapeDtypeStruct((8, 128), F32)),
        in_specs=[ANY, VMEM],
        out_specs=(VMEM, VMEM),
        scratch_shapes=[
            pltpu.VMEM((3, 1024, n), BF16),
            pltpu.VMEM((ROUNDS, 256, 1024), BF16),
            pltpu.VMEM((ROUNDS, 2, 32, 1024), BF16),
            pltpu.VMEM((ROUNDS, 2, 64, 1024), BF16),
            pltpu.VMEM((ROUNDS, 64, 1024), BF16),
            pltpu.VMEM((ROUNDS, 7, 64, 128), BF16),
            pltpu.VMEM((ROUNDS, 64, 128), F32),
            pltpu.VMEM((ROUNDS, 32, 128), BF16),
            pltpu.VMEM((ROUNDS, 32, 128), BF16),
            pltpu.VMEM((3, 128, 128), BF16),
            pltpu.VMEM((2, 128, 128), BF16),
            pltpu.VMEM((2, 64, 1024), BF16),
            pltpu.VMEM((3, 8, 128), F32),
            dma((4,)), dma((4,)), dma, dma,
            dma((ROUNDS, 2)), dma((ROUNDS, 2)), dma((ROUNDS, 2)), dma((ROUNDS, 2)),
            dma((ROUNDS,)), dma((ROUNDS,)), dma((ROUNDS,)), dma((ROUNDS,)),
            dma((3,)), dma((3,)), dma((9,)), dma((2,)), dma,
        ],
        compiler_params=pltpu.CompilerParams(has_side_effects=True, vmem_limit_bytes=40 * 2**20),
        name="gram_reduced",
    )(white, pm)


def three_parts(v):
    a = lax.reduce_precision(v, 8, 7)
    b = lax.reduce_precision(v - a, 8, 7)
    return a.astype(BF16), b.astype(BF16), (v - a - b).astype(BF16)


def shards(points, targets, inducing, whitening, mean_v, covariance, precision, natural_one, lengthscales, hypers):
    signal, noise_var = hypers[0], hypers[1]
    own_rows, own_points = inducing.shape[0], points.shape[0]
    tgt = jnp.pad(targets, (0, 1024 - own_points)).reshape(8, 128)
    all_z, pts, tgt = share(inducing.T, points.T, tgt)
    tgt_row = tgt.reshape(-1)[:own_points]
    scale = lengthscales[:, None]
    norm_x = jnp.sum(jnp.square(pts.astype(F32) / scale), axis=0)
    norm_z = jnp.sum(jnp.square(all_z / scale), axis=1).reshape(-1)
    parts = jnp.concatenate(three_parts(all_z / (scale * scale)), axis=1)
    inner = lax.dot_general(
        parts, jnp.concatenate([pts] * 3, axis=0), (((1,), (0,)), ((), ())), preferred_element_type=F32
    ).reshape(-1, own_points)
    cross = (signal * jnp.exp(-0.5 * (norm_z[:, None] + norm_x[None, :] - 2.0 * inner))).astype(BF16)
    white = jnp.dot(whitening, cross, preferred_element_type=F32).astype(BF16)
    wide = white.astype(F32)
    pm = jnp.sum(mean_v[:, None] * wide, axis=0)
    proj = jnp.sum(wide * tgt_row[None, :], axis=1)
    square = jnp.sum(wide * wide)
    gram_t, pm = gram_reduced(white, jnp.pad(pm, (0, 1024 - own_points)).reshape(8, 128))
    gram_t = gram_t.astype(F32)
    trace = jnp.sum(covariance.T * gram_t)
    fit = 0.25 * (jnp.sum(jnp.square(tgt - pm)) + signal * own_points) - square
    mine = lax.axis_index(IND)
    slots = jnp.where(jnp.arange(4)[:, None] == mine, proj[None, :], 0.0).reshape(-1)
    total = lax.psum(jnp.concatenate([slots, (trace + fit)[None]]), AXES)
    proj = lax.dynamic_slice(total, (mine * own_rows,), (own_rows,))
    count = own_points * lax.axis_size(DP_REP)
    expected_fit = -0.5 * jnp.log(2.0 * jnp.pi * noise_var) - total[-1] / (2.0 * noise_var * count)
    row_ids = mine * own_rows + jnp.arange(own_rows, dtype=jnp.int32)
    col_ids = lax.axis_index(DP_REP) * 64 + jnp.arange(64, dtype=jnp.int32)
    identity = (row_ids[None, :] == col_ids[:, None]).astype(F32)
    precision_new = (0.5 * precision.T + 0.5 * (identity + gram_t / noise_var)).T
    natural_new = 0.5 * natural_one + 0.5 * proj / noise_var
    return precision_new, natural_new, expected_fit


def solution(mesh):
    finer = Mesh(mesh.devices.reshape(8, 2, mesh.shape["rep"], 2, 2), AXES)
    return jax.shard_map(
        shards,
        mesh=finer,
        in_specs=(
            P(DP_REP, None), P(DP_REP), P(IND, None), P(IND, None), P(IND),
            P(IND, DP_REP), P(IND, DP_REP), P(IND), P(), P(),
        ),
        out_specs=(P(IND, DP_REP), P(IND), P()),
        check_vma=False,
    )
```

```python
import jax
import jax.numpy as jnp
from jax import lax
from jax.experimental import pallas as pl
from jax.experimental.pallas import tpu as pltpu
from jax.sharding import Mesh
from jax.sharding import PartitionSpec as P

AXES = ("dp_0", "dp_1", "rep", "ind_0", "ind_1")
IND = ("ind_0", "ind_1")
DP_REP = ("dp_0", "dp_1", "rep")
MESH = pl.DeviceIdType.MESH
VMEM = pl.BlockSpec(memory_space=pltpu.VMEM)
ANY = pl.BlockSpec(memory_space=pl.ANY)
F32 = jnp.float32
BF16 = jnp.bfloat16
ROUNDS = 5


def place():
    return tuple(lax.axis_index(a) for a in AXES)


def remote(src, dst, send, recv, to):
    return pltpu.make_async_remote_copy(
        src_ref=src, dst_ref=dst, send_sem=send, recv_sem=recv, device_id=to, device_id_type=MESH
    )


def greet(peers):
    barrier = pltpu.get_barrier_semaphore()
    for to in peers:
        pl.semaphore_signal(barrier, inc=1, device_id=to, device_id_type=MESH)
    pl.semaphore_wait(barrier, len(peers))


def share_kernel(z_ref, p_ref, t_ref, allz, p_out, t_out, send, recv, local):
    z, lo, y, hi, core = place()
    mine = hi * 2 + core
    other = (1 - hi) * 2 + core
    partner = (z, lo, y, hi, 1 - core)
    across = (z, 1 - lo, y, 1 - hi, core)
    swap = (z, 1 - lo, y, hi, core)
    greet((partner, across, swap))
    over = remote(z_ref, allz.at[mine], send.at[0], recv.at[0], across)
    over.start()

    @pl.when(hi == 0)
    def _():
        remote(p_ref, p_out, send.at[3], recv.at[3], swap).start()
        remote(t_ref, t_out, send.at[4], recv.at[4], swap).start()

    near = remote(z_ref, allz.at[mine], send.at[1], recv.at[1], partner)
    near.start()
    own = pltpu.make_async_copy(z_ref, allz.at[mine], local)
    own.start()

    @pl.when(hi == 1)
    def _():
        p_out[...] = p_ref[...]
        t_out[...] = t_ref[...]

    over.wait_recv()
    on = remote(allz.at[other], allz.at[other], send.at[2], recv.at[2], partner)
    on.start()
    own.wait()
    near.wait_recv()
    on.wait_recv()

    @pl.when(hi == 0)
    def _():
        remote(p_ref, p_out, send.at[3], recv.at[3], swap).wait()
        remote(t_ref, t_out, send.at[4], recv.at[4], swap).wait()

    over.wait_send()
    near.wait_send()
    on.wait_send()


def share(z_t, p_t, tgt):
    return pl.pallas_call(
        share_kernel,
        out_shape=(
            jax.ShapeDtypeStruct((4, *z_t.shape), F32),
            jax.ShapeDtypeStruct(p_t.shape, BF16),
            jax.ShapeDtypeStruct(tgt.shape, F32),
        ),
        in_specs=[VMEM] * 3,
        out_specs=(VMEM, VMEM, VMEM),
        scratch_shapes=[
            pltpu.SemaphoreType.DMA((5,)),
            pltpu.SemaphoreType.DMA((5,)),
            pltpu.SemaphoreType.DMA,
        ],
        compiler_params=pltpu.CompilerParams(has_side_effects=True, collective_id=0),
        name="share",
    )(z_t, p_t, tgt)


def round_of(t):
    is_b = t // 3
    is_h = (t // 2) * (1 - is_b)
    g = 2 * ((t + is_b) % 2) * (1 - is_h)
    return is_b, is_h, g


def gram_kernel(
    noise, white, pm_ref, proj_ref, tgt, square, cov, prec, nat, out, nat_out, sum_out,
    wbuf, pay, y1, y2, zs, zr, xk, xs, xr, qay, qx, qs, q1, q2, qz, qr, fin, fint, own, pmr, vec, vy, vz, vx,
    g_s, g_r, p_s, p_r, y1_s, y1_r, y2_s, y2_r, z_s, z_r, x_s, x_r,
    qx_s, qx_r, q1_s, q1_r, q2_s, q2_r, qz_s, qz_r, pm_s, pm_r, f_s, own_sem, w_sem, v_s, v_r,
):
    z, lo, y, hi, core = place()
    mine = hi * 2 + core
    yp, ym, y2p = (y + 1) % 4, (y + 3) % 4, (y + 2) % 4
    partner = (z, lo, y, hi, 1 - core)
    gather_to = (z, 1 - lo, y, 1 - hi, (core + 1 - hi) % 2)

    load = pltpu.make_async_copy(white, wbuf.at[core], w_sem)
    load.start()
    line = [
        (z, (lo + d // 4) % 2, y, (hi + (d // 2) % 2) % 2, (core + d % 2) % 2) for d in range(1, 8)
    ]
    over_y = [(z, lo, (y + d) % 4, hi, core) for d in range(1, 4)]
    over_z = [((z + d) % 8, lo, y, hi, core) for d in range(1, 8)]
    greet(over_y + over_z + line)

    def vec_into(k):
        return (vy.at[0], vz.at[0], vx.at[pl.ds(0, 1)], vy.at[1], vz.at[1], vx.at[pl.ds(1, 7)])[k]

    def vec_send(k, src):
        for i, to in enumerate((over_y, over_z, [(z, 1 - lo, y, hi, core)], over_y, over_z, line)[k]):
            remote(src, vec_into(k).at[i], v_s.at[k], v_r.at[k], to).start()

    def vec_sum(k, src):
        into = vec_into(k)
        remote(into, into, v_s.at[k], v_r.at[k], partner).wait_recv()
        total = src[...]
        for i in range(into.shape[0]):
            total = total + into[i]
        return total

    vec_send(0, proj_ref)
    pm_to = (partner, (z, 1 - lo, y, 1 - hi, core), (z, 1 - lo, y, 1 - hi, 1 - core))
    pm_copies = [remote(pm_ref, pmr.at[k], pm_s.at[k], pm_r.at[k], to) for k, to in enumerate(pm_to)]
    for c in pm_copies:
        c.start()
    load.wait()

    def gather_piece(g, k):
        rows = pl.ds(pl.multiple_of(k * 128 + 32 * g, 32), 32)
        return remote(wbuf.at[core, rows], wbuf.at[2, rows], g_s.at[g], g_r.at[g], gather_to)

    def gather_start(g, _):
        lax.fori_loop(0, 8, lambda k, c: (gather_piece(g, k).start(), c)[1], 0)
        return 0

    lax.fori_loop(0, 4, gather_start, 0)
    to_partner = remote(wbuf.at[core], wbuf.at[core], p_s, p_r, partner)
    to_partner.start()

    def gather_all(g):
        rows = pl.ds(0, 256)
        return remote(wbuf.at[core, rows], wbuf.at[2, rows], g_s.at[g], g_r.at[g], gather_to)

    up_y, down_y = (z, lo, yp, hi, core), (z, lo, ym, hi, core)
    over_x = (z, 1 - lo, y, hi, core)

    def block(k, size):
        return pl.ds(pl.multiple_of(k * size, size), size)

    def y1_copies(t):
        return (
            remote(pay.at[t, block(2 * y2p, 32)], y1.at[t, 0], y1_s.at[t, 0], y1_r.at[t, 0], up_y),
            remote(pay.at[t, block(2 * y2p + 1, 32)], y1.at[t, 1], y1_s.at[t, 1], y1_r.at[t, 1], down_y),
        )

    def y2_copies(t):
        return (
            remote(pay.at[t, block(yp, 64)], y2.at[t, 0], y2_s.at[t, 0], y2_r.at[t, 0], up_y),
            remote(pay.at[t, block(ym, 64)], y2.at[t, 1], y2_s.at[t, 1], y2_r.at[t, 1], down_y),
        )

    def z_send(t):
        for d in range(1, 8):
            to = (z + d) % 8
            remote(zs.at[t, :, block(to, 128)], zr.at[t, d - 1], z_s.at[t], z_r.at[t], over_z[d - 1]).start()

    def z_all(t):
        return remote(zr.at[t], zr.at[t], z_s.at[t], z_r.at[t], over_x)

    def x_copy(t):
        return remote(xs.at[t], xr.at[t], x_s.at[t], x_r.at[t], over_x)

    def qx_copy(t):
        return remote(qay.at[t, block(1 - lo, 128)], qx.at[t], qx_s.at[t], qx_r.at[t], over_x)

    def q1_copies(t):
        return (
            remote(qs.at[t, block(2 * y2p, 16)], q1.at[t, 0], q1_s.at[t, 0], q1_r.at[t, 0], up_y),
            remote(qs.at[t, block(2 * y2p + 1, 16)], q1.at[t, 1], q1_s.at[t, 1], q1_r.at[t, 1], down_y),
        )

    def q2_copies(t):
        return (
            remote(qs.at[t, block(yp, 32)], q2.at[t, 0], q2_s.at[t, 0], q2_r.at[t, 0], up_y),
            remote(qs.at[t, block(ym, 32)], q2.at[t, 1], q2_s.at[t, 1], q2_r.at[t, 1], down_y),
        )

    def qz_send(t):
        for d in range(1, 8):
            to = (z + d) % 8
            remote(qz.at[t, :, block(to, 128)], qr.at[t, d - 1], qz_s.at[t], qz_r.at[t], over_z[d - 1]).start()

    def qz_all(t):
        return remote(qr.at[t], qr.at[t], qz_s.at[t], qz_r.at[t], over_x)

    def slab(t, g, groups, into):
        is_b, is_h, _ = round_of(t)
        plain = 1 - is_h
        left = is_b * 2 + is_h + plain * (1 - is_b) * core
        right = plain * core
        shift = g + is_h * 2 * core
        a = jnp.concatenate([wbuf[left, pl.ds(pl.multiple_of(k * 128 + 32 * shift, 32), 32), :] for k in groups], axis=0)
        for j in range(4):
            b = wbuf[right, j * 256 : (j + 1) * 256, :]
            part = lax.dot_general(a, b, (((1,), (1,)), ((), ())), preferred_element_type=F32)
            into[t, :, j * 256 : (j + 1) * 256] = part.astype(BF16)

    def compute(t):
        is_b, is_h, g = round_of(t)

        @pl.when(is_h == 1)
        def _():
            to_partner.wait_recv()

        @pl.when(is_b == 1)
        def _():
            gather_all(g + 1).wait_recv()

        slab(t, g + 1, (0, 2, 4, 6, 1, 3, 5, 7), qay)
        qx_copy(t).start()

        @pl.when(is_b == 1)
        def _():
            gather_all(g).wait_recv()

        slab(t, g, range(8), pay)
        for c in y1_copies(t):
            c.start()

    def after_1(t):
        qx_copy(t).wait_recv()
        qs[t] = (qay[t, block(lo, 128), :].astype(F32) + qx[t].astype(F32)).astype(BF16)
        for c in q1_copies(t):
            c.start()
        for k, c in enumerate(y1_copies(t)):
            c.wait_recv()
            rows = block(2 * (yp, ym)[k] + k, 32)
            pay[t, rows, :] = (pay[t, rows, :].astype(F32) + y1[t, k].astype(F32)).astype(BF16)
        for c in y2_copies(t):
            c.start()

    def after_2(t):
        for k, c in enumerate(q1_copies(t)):
            c.wait_recv()
            rows = block(2 * (yp, ym)[k] + k, 16)
            qs[t, rows, :] = (qs[t, rows, :].astype(F32) + q1[t, k].astype(F32)).astype(BF16)
        for c in q2_copies(t):
            c.start()
        for c in y2_copies(t):
            c.wait_recv()
        total = pay[t, block(y, 64), :].astype(F32) + y2[t, 0].astype(F32) + y2[t, 1].astype(F32)
        zs[t] = total.astype(BF16)
        z_send(t)

    def after_3(t):
        for c in q2_copies(t):
            c.wait_recv()
        total = qs[t, block(y, 32), :].astype(F32) + q2[t, 0].astype(F32) + q2[t, 1].astype(F32)
        qz[t] = total.astype(BF16)
        qz_send(t)
        z_all(t).wait_recv()
        total = zs[t, :, block(z, 128)].astype(F32)
        for d in range(7):
            total = total + zr[t, d].astype(F32)
        xk[t] = total
        xs[t] = xk[t, block(1 - lo, 32), :].astype(BF16)
        x_copy(t).start()

    def after_4(t):
        is_b, is_h, g = round_of(t)
        slot = is_b + 2 * is_h
        row = g + is_h * core * 2
        x_copy(t).wait_recv()
        total = xk[t, block(lo, 32), :] + xr[t].astype(F32)
        fin[slot, block(row, 32), :] = total.astype(BF16)
        qz_all(t).wait_recv()
        total = qz[t, :, block(z, 128)].astype(F32)
        for d in range(7):
            total = total + qr[t, d].astype(F32)
        fin[slot, block(row + 1, 32), :] = total.astype(BF16)

    zero = jnp.zeros((128, 128), BF16)
    fin[2] = zero

    def step(t, carry):
        @pl.when(t == 2)
        def _():
            vec[0] = vec_sum(0, proj_ref)
            vec_send(1, vec.at[0])

        @pl.when(t == 4)
        def _():
            vec[1] = vec_sum(1, vec.at[0])
            vec_send(2, vec.at[1])

        for lag, work in ((4, after_4), (3, after_3), (2, after_2), (1, after_1), (0, compute)):

            @pl.when((t >= lag) & (t < ROUNDS + lag))
            def _(lag=lag, work=work):
                work(t - lag)

        return carry

    lax.fori_loop(0, ROUNDS + 4, step, 0)

    fint[0] = fin[1].astype(F32).T.astype(BF16)
    fint[1] = fin[2].astype(F32).T.astype(BF16)

    nxt = (1 - hi) * 2 + (core + hi) % 2
    low, high = hi * 2, hi * 2 + 1
    me = (((z * 2 + lo) * 4 + y) * 2 + hi) * 2 + core
    direct = pl.ds(pl.multiple_of(z * 128, 128), 128)
    mirror = pl.ds(pl.multiple_of(256 * y + 128 * lo, 128), 128)

    def owner(q, ind):
        return (q // 8, (q // 4) % 2, q % 4, ind // 2, ind % 2)

    sends = []
    for e in range(2):
        rows = slice(64 * e, 64 * e + 64)
        sends.append((fin.at[0, rows], own.at[0, :, direct], own_sem.at[0], owner(16 * mine + 4 * y + 2 * lo + e, mine)))
        sends.append((fin.at[1, rows], own.at[0, :, direct], own_sem.at[0], owner(16 * nxt + 4 * y + 2 * lo + e, mine)))
        sends.append((fint.at[0, rows], own.at[0, :, mirror], own_sem.at[0], owner(16 * mine + 2 * z + e, nxt)))
        sends.append((fint.at[1, rows], own.at[core, :, mirror], own_sem.at[core], owner(16 * low + 2 * z + e, high)))
    half = pl.ds(pl.multiple_of(64 * core, 64), 64)
    sends.append((fin.at[2, half], own.at[0, :, direct], own_sem.at[0], owner(16 * high + 4 * y + 2 * lo + core, low)))

    def flat(d):
        return (((d[0] * 2 + d[1]) * 4 + d[2]) * 2 + d[3]) * 2 + d[4]

    for k, (src, dst, sem, to) in enumerate(sends):

        @pl.when(flat(to) != me)
        def _(k=k, src=src, dst=dst, sem=sem, to=to):
            remote(src, dst, f_s.at[k], sem, to).start()

        @pl.when(flat(to) == me)
        def _(src=src, dst=dst, sem=sem):
            pltpu.make_async_copy(src, dst, sem).start()

    for c in pm_copies:
        c.wait_recv()
    resid = tgt[...] - (pm_ref[...] + pmr[0] + pmr[1] + pmr[2])
    per_noise = 0.5 / noise[0]
    nat_out[...] = 0.5 * nat[...] + vec_sum(2, vec.at[1]) * per_noise

    pltpu.make_async_copy(own.at[0], own.at[0], own_sem.at[0]).wait()
    both = core * (1 - jnp.minimum(jnp.abs(z // 2 - low), 1))

    @pl.when(both == 1)
    def _():
        pltpu.make_async_copy(own.at[1], own.at[1], own_sem.at[1]).wait()
        own[0] = own[0] + own[1]

    total = 0.25 * resid * resid - square[...]
    for j in range(8):
        cols = slice(128 * j, 128 * j + 128)
        for i in range(8):
            rows = slice(8 * i, 8 * i + 8)
            total = total + cov[rows, cols] * own[0, rows, cols].astype(F32)
    vec[2] = total
    vec_send(3, vec.at[2])
    gap = ((z * 2 + lo) * 4 + y) * 64 - mine * 1024
    for i in range(8):
        rows = slice(8 * i, 8 * i + 8)
        shape = (8, 1024)
        same = lax.broadcasted_iota(jnp.int32, shape, 1) - lax.broadcasted_iota(jnp.int32, shape, 0) == gap + 8 * i
        out[rows] = 0.5 * prec[rows] + (jnp.where(same, 0.5, 0.0) + own[0, rows].astype(F32) * per_noise)
    vec[3] = vec_sum(3, vec.at[2])
    vec_send(4, vec.at[3])
    vec[4] = vec_sum(4, vec.at[3])
    vec_send(5, vec.at[4])
    sum_out[...] = vec_sum(5, vec.at[4])
    for k in range(6):
        into = vec_into(k)
        remote(into, into, v_s.at[k], v_r.at[k], partner).wait_send()

    for k, (src, dst, sem, to) in enumerate(sends):

        @pl.when(flat(to) != me)
        def _(k=k, src=src, dst=dst, sem=sem, to=to):
            remote(src, dst, f_s.at[k], sem, to).wait_send()

    for c in pm_copies:
        c.wait_send()
    to_partner.wait_send()

    def drain(t, carry):
        for c in y1_copies(t) + y2_copies(t) + q1_copies(t) + q2_copies(t):
            c.wait_send()
        for c in (z_all(t), x_copy(t), qz_all(t), qx_copy(t)):
            c.wait_send()
        return carry

    lax.fori_loop(0, ROUNDS, drain, 0)
    lax.fori_loop(0, 4, lambda g, c: (gather_all(g).wait_send(), c)[1], 0)


def gram_reduced(noise, white, pm, proj, tgt, square, cov, prec, nat):
    dma = pltpu.SemaphoreType.DMA
    n = white.shape[1]
    return pl.pallas_call(
        gram_kernel,
        out_shape=tuple(jax.ShapeDtypeStruct(s, F32) for s in ((64, 1024), (8, 128), (8, 128))),
        in_specs=[pl.BlockSpec(memory_space=pltpu.SMEM), ANY] + [VMEM] * 7,
        out_specs=(VMEM, VMEM, VMEM),
        scratch_shapes=[
            pltpu.VMEM((3, 1024, n), BF16),
            pltpu.VMEM((ROUNDS, 256, 1024), BF16),
            pltpu.VMEM((ROUNDS, 2, 32, 1024), BF16),
            pltpu.VMEM((ROUNDS, 2, 64, 1024), BF16),
            pltpu.VMEM((ROUNDS, 64, 1024), BF16),
            pltpu.VMEM((ROUNDS, 7, 64, 128), BF16),
            pltpu.VMEM((ROUNDS, 64, 128), F32),
            pltpu.VMEM((ROUNDS, 32, 128), BF16),
            pltpu.VMEM((ROUNDS, 32, 128), BF16),
            pltpu.VMEM((ROUNDS, 256, 1024), BF16),
            pltpu.VMEM((ROUNDS, 128, 1024), BF16),
            pltpu.VMEM((ROUNDS, 128, 1024), BF16),
            pltpu.VMEM((ROUNDS, 2, 16, 1024), BF16),
            pltpu.VMEM((ROUNDS, 2, 32, 1024), BF16),
            pltpu.VMEM((ROUNDS, 32, 1024), BF16),
            pltpu.VMEM((ROUNDS, 7, 32, 128), BF16),
            pltpu.VMEM((3, 128, 128), BF16),
            pltpu.VMEM((2, 128, 128), BF16),
            pltpu.VMEM((2, 64, 1024), BF16),
            pltpu.VMEM((3, 8, 128), F32),
            pltpu.VMEM((5, 8, 128), F32),
            pltpu.VMEM((2, 3, 8, 128), F32),
            pltpu.VMEM((2, 7, 8, 128), F32),
            pltpu.VMEM((8, 8, 128), F32),
            dma((4,)), dma((4,)), dma, dma,
            dma((ROUNDS, 2)), dma((ROUNDS, 2)), dma((ROUNDS, 2)), dma((ROUNDS, 2)),
            dma((ROUNDS,)), dma((ROUNDS,)), dma((ROUNDS,)), dma((ROUNDS,)),
            dma((ROUNDS,)), dma((ROUNDS,)), dma((ROUNDS, 2)), dma((ROUNDS, 2)),
            dma((ROUNDS, 2)), dma((ROUNDS, 2)), dma((ROUNDS,)), dma((ROUNDS,)),
            dma((3,)), dma((3,)), dma((9,)), dma((2,)), dma, dma((6,)), dma((6,)),
        ],
        compiler_params=pltpu.CompilerParams(has_side_effects=True, collective_id=1, vmem_limit_bytes=40 * 2**20),
        name="gram_reduced",
    )(noise, white, pm, proj, tgt, square, cov, prec, nat)


def three_parts(v):
    a = lax.reduce_precision(v, 8, 7)
    b = lax.reduce_precision(v - a, 8, 7)
    return a.astype(BF16), b.astype(BF16), (v - a - b).astype(BF16)


def shards(points, targets, inducing, whitening, mean_v, covariance, precision, natural_one, lengthscales, hypers):
    signal, noise_var = hypers[0], hypers[1]
    own_rows, own_points = inducing.shape[0], points.shape[0]
    tgt = jnp.pad(targets, (0, 1024 - own_points)).reshape(8, 128)
    all_z, pts, tgt = share(inducing.T, points.T, tgt)
    tgt_row = tgt.reshape(-1)[:own_points]
    scale = lengthscales[:, None]
    norm_x = jnp.sum(jnp.square(pts.astype(F32) / scale), axis=0)
    norm_z = jnp.sum(jnp.square(all_z / scale), axis=1).reshape(-1)
    parts = jnp.concatenate(three_parts(all_z / (scale * scale)), axis=1)
    inner = lax.dot_general(
        parts, jnp.concatenate([pts] * 3, axis=0), (((1,), (0,)), ((), ())), preferred_element_type=F32
    ).reshape(-1, own_points)
    cross = (signal * jnp.exp(-0.5 * (norm_z[:, None] + norm_x[None, :] - 2.0 * inner))).astype(BF16)
    white = jnp.dot(whitening, cross, preferred_element_type=F32).astype(BF16)
    wide = white.astype(F32)
    pm = jnp.sum(mean_v[:, None] * wide, axis=0)
    proj = jnp.sum(wide * tgt_row[None, :], axis=1)
    square = jnp.sum(wide * wide)
    precision_new, natural_new, total = gram_reduced(
        noise_var[None],
        white,
        jnp.pad(pm, (0, 1024 - own_points)).reshape(8, 128),
        proj.reshape(8, 128),
        tgt,
        jnp.full((8, 128), square / 1024, F32),
        covariance.T,
        precision.T,
        natural_one.reshape(8, 128),
    )
    count = own_points * lax.axis_size(DP_REP)
    expected_fit = -0.5 * jnp.log(2.0 * jnp.pi * noise_var) - (jnp.sum(total) + signal * count) / (
        2.0 * noise_var * count
    )
    return precision_new.T, natural_new.reshape(own_rows), expected_fit


def solution(mesh):
    finer = Mesh(mesh.devices.reshape(8, 2, mesh.shape["rep"], 2, 2), AXES)
    return jax.shard_map(
        shards,
        mesh=finer,
        in_specs=(
            P(DP_REP, None), P(DP_REP), P(IND, None), P(IND, None), P(IND),
            P(IND, DP_REP), P(IND, DP_REP), P(IND), P(), P(),
        ),
        out_specs=(P(IND, DP_REP), P(IND), P()),
        check_vma=False,
    )
```

```python
import jax
import jax.numpy as jnp
from jax import lax
from jax.experimental import pallas as pl
from jax.experimental.pallas import tpu as pltpu
from jax.sharding import Mesh
from jax.sharding import PartitionSpec as P

AXES = ("dp_0", "dp_1", "rep", "ind_0", "ind_1")
IND = ("ind_0", "ind_1")
DP_REP = ("dp_0", "dp_1", "rep")
MESH = pl.DeviceIdType.MESH
VMEM = pl.BlockSpec(memory_space=pltpu.VMEM)
ANY = pl.BlockSpec(memory_space=pl.ANY)
F32 = jnp.float32
BF16 = jnp.bfloat16
ROUNDS = 5


def place():
    return tuple(lax.axis_index(a) for a in AXES)


def remote(src, dst, send, recv, to):
    return pltpu.make_async_remote_copy(
        src_ref=src, dst_ref=dst, send_sem=send, recv_sem=recv, device_id=to, device_id_type=MESH
    )


def parts_of(v):
    a = v.astype(BF16)
    b = (v - a.astype(F32)).astype(BF16)
    return a, b, (v - a.astype(F32) - b.astype(F32)).astype(BF16)


def tile_of(v):
    row = lax.broadcasted_iota(jnp.int32, (16, v.shape[1]), 0)
    tile = jnp.zeros((16, v.shape[1]), F32)
    for k, part in enumerate(parts_of(v)):
        tile = jnp.where(row == k, part.astype(F32), tile)
    return tile.astype(BF16)


def dot(a, b, dims):
    return lax.dot_general(a, b, ((dims[:1], dims[1:]), ((), ())), preferred_element_type=F32)


def round_of(t):
    is_b = t // 3
    is_h = (t // 2) * (1 - is_b)
    g = 2 * ((t + is_b) % 2) * (1 - is_h)
    return is_b, is_h, g


def kernel(
    hypers, ind_t, pts_in, tgt_in, scale_in, mean, whitening, cov, prec, nat, out, nat_out, fit_out,
    zall, pts, tgt, wv, cross, acc, square, pmv, covb,
    wbuf, pay, y1, y2, zs, zr, xk, xs, xr, qay, qx, qs, q1, q2, qz, qr, fin, fint, own, pmr, vec, vy, vz, vx, va, vb,
    i_s, i_r, c_s, cov_s, cov_r,
    g_s, g_r, p_s, p_r, y1_s, y1_r, y2_s, y2_r, z_s, z_r, x_s, x_r,
    qx_s, qx_r, q1_s, q1_r, q2_s, q2_r, qz_s, qz_r, pm_s, pm_r, f_s, own_sem, v_s, v_r,
):
    z, lo, y, hi, core = place()
    mine = hi * 2 + core
    yp, ym, y2p = (y + 1) % 4, (y + 3) % 4, (y + 2) % 4
    partner = (z, lo, y, hi, 1 - core)
    gather_to = (z, 1 - lo, y, 1 - hi, (core + 1 - hi) % 2)

    count = pts.shape[1]
    cut = wv.shape[2]
    w_copies = [
        pltpu.make_async_copy(
            whitening.at[:, pl.ds(pl.multiple_of((hi + h - 2 * hi * h) * cut, cut), cut)], wv.at[h], c_s.at[h]
        )
        for h in range(2)
    ]
    for c in w_copies:
        c.start()
    line = [
        (z, (lo + d // 4) % 2, y, (hi + (d // 2) % 2) % 2, (core + d % 2) % 2) for d in range(1, 8)
    ]
    over_y = [(z, lo, (y + d) % 4, hi, core) for d in range(1, 4)]
    over_z = [((z + d) % 8, lo, y, hi, core) for d in range(1, 8)]
    low, high = hi * 2, hi * 2 + 1
    nxt = (1 - hi) * 2 + (core + hi) % 2
    prv = (1 - hi) * 2 + (core + 1 - hi) % 2

    def owner(q, ind):
        return (q // 8, (q // 4) % 2, q % 4, ind // 2, ind % 2)

    def flat(d):
        return (((d[0] * 2 + d[1]) * 4 + d[2]) * 2 + d[3]) * 2 + d[4]

    def equal(a, b):
        return 1 - jnp.minimum(jnp.abs(a - b), 1)

    me = flat(place())
    here = 4 * y + 2 * lo
    holders = (
        [owner(16 * mine + here + e, mine) for e in range(2)]
        + [owner(16 * nxt + here + e, mine) for e in range(2)]
        + [owner(16 * mine + 2 * z + e, nxt) for e in range(2)]
        + [owner(16 * high + here + core, low)]
        + [owner(16 * low + 2 * z + e, high) for e in range(2)]
    )
    own_group, own_q = z // 2, (z % 2) * 8 + lo * 4 + y
    is_d, is_n, is_p = equal(own_group, mine), equal(own_group, nxt), equal(own_group, prv)
    is_s = 1 - is_d - is_n - is_p
    mirrored = is_p + is_s * core
    both = is_s * core

    def cov_target(i, second):
        e = own_q % 2
        to_core = is_p * (own_group % 2) + is_s * ((1 - core) * e + core * second) + (1 - is_p - is_s) * core
        to = (
            (1 - mirrored) * i + mirrored * (own_q // 2),
            (1 - mirrored) * ((own_q // 2) % 2) + mirrored * (i % 2),
            (1 - mirrored) * (own_q // 4) + mirrored * (i // 2),
            is_p * (own_group // 2) + (1 - is_p) * hi,
            to_core,
        )
        slot = is_d * e + is_n * (2 + e) + is_p * (4 + e) + is_s * ((1 - core) * 6 + core * (7 + e))
        return to, cov.at[:, pl.ds(pl.multiple_of(i * 128, 128), 128)], covb.at[slot]

    barrier = pltpu.get_barrier_semaphore()
    arrivals = 17 + 8 * (1 + both)
    for to in over_y + over_z + line:
        pl.semaphore_signal(barrier, inc=1, device_id=to, device_id_type=MESH)
    for to in holders:
        arrivals = arrivals - equal(flat(to), me)

        @pl.when(flat(to) != me)
        def _(to=to):
            pl.semaphore_signal(barrier, inc=1, device_id=to, device_id_type=MESH)

    pl.semaphore_wait(barrier, arrivals)

    over_a = [((z + d) % 8, lo, y, hi, (core + c) % 2) for d in range(8) for c in range(2) if d + c]
    over_b = [
        (z, (lo + a) % 2, (y + d) % 4, (hi + b) % 2, core)
        for d in range(4)
        for a in range(2)
        for b in range(2)
        if d + a + b
    ]

    def cov_sends(second, act):
        def one(i, carry):
            to, src, dst = cov_target(i, second)

            @pl.when(flat(to) != me)
            def _():
                act(remote(src, dst, cov_s.at[8 * second + i], cov_r, to), True)

            @pl.when(flat(to) == me)
            def _():
                act(pltpu.make_async_copy(src, dst, cov_r), False)

            return carry

        lax.fori_loop(0, 8, one, 0)

    def cov_start(copy, far):
        copy.start()

    def cov_sent(copy, far):
        if far:
            copy.wait_send()

    def vec_into(k):
        return (vy, vz, vx, va, vb)[k]

    def vec_send(k, src):
        for i, to in enumerate((over_y, over_z, [(z, 1 - lo, y, hi, core)], over_a, over_b)[k]):
            remote(src, vec_into(k).at[i], v_s.at[k], v_r.at[k], to).start()

    def vec_sum(k, src):
        into = vec_into(k)
        remote(into, into, v_s.at[k], v_r.at[k], partner).wait_recv()
        total = src[...]
        return total + sum(into[i] for i in range(into.shape[0]))

    other = (1 - hi) * 2 + core
    across = (z, 1 - lo, y, 1 - hi, core)
    swap = (z, 1 - lo, y, hi, core)
    over = remote(ind_t, zall.at[mine], i_s.at[0], i_r.at[0], across)
    near = remote(ind_t, zall.at[mine], i_s.at[1], i_r.at[1], partner)
    on = remote(zall.at[other], zall.at[other], i_s.at[2], i_r.at[2], partner)
    swaps = (
        remote(pts_in, pts, i_s.at[3], i_r.at[3], swap),
        remote(tgt_in, tgt, i_s.at[4], i_r.at[4], swap),
    )

    @pl.when(hi == 0)
    def _():
        for c in swaps:
            c.start()

    over.start()
    near.start()
    own_z = pltpu.make_async_copy(ind_t, zall.at[mine], c_s.at[2])
    own_z.start()
    cov_sends(0, cov_start)

    @pl.when(both == 1)
    def _():
        cov_sends(1, cov_start)

    @pl.when(hi == 1)
    def _():
        pts[...] = pts_in[...]
        tgt[...] = tgt_in[...]

    own_z.wait()

    @pl.when(hi == 0)
    def _():
        for c in swaps:
            c.wait()

    diagonal = lax.broadcasted_iota(jnp.int32, (64, 64), 0) == lax.broadcasted_iota(jnp.int32, (64, 64), 1)
    scale = jnp.sum(jnp.where(diagonal, jnp.broadcast_to(scale_in[...], (64, 64)), 0.0), axis=1, keepdims=True)
    scales = jnp.broadcast_to(scale, (64, count))
    t_row = jnp.concatenate([tgt[j : j + 1, :] for j in range(count // 128)], axis=1)
    norm_x = 0.5 * jnp.sum(jnp.square(pts[...].astype(F32) / scales), axis=0, keepdims=True)
    three = lax.broadcasted_iota(jnp.int32, (16, count), 0) < 3
    p_mat = jnp.concatenate([pts[...]] * 3 + [jnp.where(three, 1.0, 0.0).astype(BF16)], axis=0)

    def cross_rows(held, half, at):
        def piece(j, carry):
            cols = pl.ds(pl.multiple_of(j * 256, 256), 256)
            zt = zall[held, :, cols]
            s = jnp.broadcast_to(scale, (64, 256))
            zs_ = zt / s
            norm = tile_of(-0.5 * jnp.sum(zs_ * zs_, axis=0, keepdims=True))
            z_mat = jnp.concatenate([*parts_of(zs_ / s), norm], axis=0)
            power = dot(z_mat, p_mat, (0, 0)) - norm_x
            rows = pl.ds(pl.multiple_of(at * 1024 + j * 256, 256), 256)
            cross[half, rows, :] = (hypers[0] * jnp.exp(power)).astype(BF16)
            return carry

        lax.fori_loop(0, 4, piece, 0)

    cross_rows(mine, 0, core)
    near.wait_recv()
    cross_rows(hi * 2 + 1 - core, 0, 1 - core)
    w_copies[0].wait()

    def first_half(i, carry):
        rows = pl.ds(pl.multiple_of(i * 256, 256), 256)
        for j in range(count // 256):
            cols = slice(256 * j, 256 * j + 256)
            acc[rows, cols] = dot(wv[0, rows, :], cross[0, :, cols], (1, 0))
        return carry

    over.wait_recv()
    on.start()
    lax.fori_loop(0, 4, first_half, 0)
    cross_rows(other, 1, core)
    on.wait_recv()
    cross_rows((1 - hi) * 2 + 1 - core, 1, 1 - core)
    w_copies[1].wait()
    square[...] = jnp.zeros((8, 128), F32)

    def gather_piece(g, k):
        rows = pl.ds(pl.multiple_of(k * 128 + 32 * g, 32), 32)
        return remote(wbuf.at[core, rows], wbuf.at[2, rows], g_s.at[g], g_r.at[g], gather_to)

    def second_half(g, carry):
        rows = [pl.ds(pl.multiple_of(k * 128 + 32 * g, 32), 32) for k in range(8)]
        a = jnp.concatenate([wv[1, r, :] for r in rows], axis=0)
        for j in range(count // 256):
            cols = slice(256 * j, 256 * j + 256)
            part = dot(a, cross[1, :, cols], (1, 0)) + jnp.concatenate([acc[r, cols] for r in rows], axis=0)
            part = part.astype(BF16)
            for k, r in enumerate(rows):
                wbuf[core, r, cols] = part[32 * k : 32 * k + 32]
            wide = part.astype(F32)
            both = jnp.sum((wide * wide).reshape(32, 8, 256), axis=0)
            square[...] += both[:, :128] + both[:, 128:]
        lax.fori_loop(0, 8, lambda k, c: (gather_piece(g, k).start(), c)[1], 0)
        return carry

    lax.fori_loop(0, 4, second_half, 0)
    to_partner = remote(wbuf.at[core], wbuf.at[core], p_s, p_r, partner)
    to_partner.start()
    m_row = jnp.concatenate([mean[j : j + 1, :] for j in range(8)], axis=1)
    pmv[...] = jnp.sum(dot(tile_of(m_row), wbuf[core], (1, 0)), axis=0, keepdims=True)
    pm_to = (partner, (z, 1 - lo, y, 1 - hi, core), (z, 1 - lo, y, 1 - hi, 1 - core))
    pm_copies = [remote(pmv, pmr.at[k], pm_s.at[k], pm_r.at[k], to) for k, to in enumerate(pm_to)]
    for c in pm_copies:
        c.start()
    proj = jnp.sum(dot(tile_of(t_row), wbuf[core], (1, 1)), axis=0, keepdims=True)
    vec[2] = jnp.concatenate([proj[:, 128 * j : 128 * j + 128] for j in range(8)], axis=0)
    vec_send(0, vec.at[2])

    def gather_all(g):
        rows = pl.ds(0, 256)
        return remote(wbuf.at[core, rows], wbuf.at[2, rows], g_s.at[g], g_r.at[g], gather_to)

    up_y, down_y = (z, lo, yp, hi, core), (z, lo, ym, hi, core)
    over_x = (z, 1 - lo, y, hi, core)

    def block(k, size):
        return pl.ds(pl.multiple_of(k * size, size), size)

    def y1_copies(t):
        return (
            remote(pay.at[t, block(2 * y2p, 32)], y1.at[t, 0], y1_s.at[t, 0], y1_r.at[t, 0], up_y),
            remote(pay.at[t, block(2 * y2p + 1, 32)], y1.at[t, 1], y1_s.at[t, 1], y1_r.at[t, 1], down_y),
        )

    def y2_copies(t):
        return (
            remote(pay.at[t, block(yp, 64)], y2.at[t, 0], y2_s.at[t, 0], y2_r.at[t, 0], up_y),
            remote(pay.at[t, block(ym, 64)], y2.at[t, 1], y2_s.at[t, 1], y2_r.at[t, 1], down_y),
        )

    def z_send(t):
        for d in range(1, 8):
            to = (z + d) % 8
            remote(zs.at[t, :, block(to, 128)], zr.at[t, d - 1], z_s.at[t], z_r.at[t], over_z[d - 1]).start()

    def z_all(t):
        return remote(zr.at[t], zr.at[t], z_s.at[t], z_r.at[t], over_x)

    def x_copy(t):
        return remote(xs.at[t], xr.at[t], x_s.at[t], x_r.at[t], over_x)

    def qx_copy(t):
        return remote(qay.at[t, block(1 - lo, 128)], qx.at[t], qx_s.at[t], qx_r.at[t], over_x)

    def q1_copies(t):
        return (
            remote(qs.at[t, block(2 * y2p, 16)], q1.at[t, 0], q1_s.at[t, 0], q1_r.at[t, 0], up_y),
            remote(qs.at[t, block(2 * y2p + 1, 16)], q1.at[t, 1], q1_s.at[t, 1], q1_r.at[t, 1], down_y),
        )

    def q2_copies(t):
        return (
            remote(qs.at[t, block(yp, 32)], q2.at[t, 0], q2_s.at[t, 0], q2_r.at[t, 0], up_y),
            remote(qs.at[t, block(ym, 32)], q2.at[t, 1], q2_s.at[t, 1], q2_r.at[t, 1], down_y),
        )

    def qz_send(t):
        for d in range(1, 8):
            to = (z + d) % 8
            remote(qz.at[t, :, block(to, 128)], qr.at[t, d - 1], qz_s.at[t], qz_r.at[t], over_z[d - 1]).start()

    def qz_all(t):
        return remote(qr.at[t], qr.at[t], qz_s.at[t], qz_r.at[t], over_x)

    def slab(t, g, groups, into):
        is_b, is_h, _ = round_of(t)
        plain = 1 - is_h
        left = is_b * 2 + is_h + plain * (1 - is_b) * core
        right = plain * core
        shift = g + is_h * 2 * core
        a = jnp.concatenate([wbuf[left, pl.ds(pl.multiple_of(k * 128 + 32 * shift, 32), 32), :] for k in groups], axis=0)
        for j in range(4):
            b = wbuf[right, j * 256 : (j + 1) * 256, :]
            part = dot(a, b, (1, 1))
            into[t, :, j * 256 : (j + 1) * 256] = part.astype(BF16)

    def compute(t):
        is_b, is_h, g = round_of(t)

        @pl.when(is_h == 1)
        def _():
            to_partner.wait_recv()

        @pl.when(is_b == 1)
        def _():
            gather_all(g + 1).wait_recv()

        slab(t, g + 1, (0, 2, 4, 6, 1, 3, 5, 7), qay)
        qx_copy(t).start()

        @pl.when(is_b == 1)
        def _():
            gather_all(g).wait_recv()

        slab(t, g, range(8), pay)
        for c in y1_copies(t):
            c.start()

    def after_1(t):
        qx_copy(t).wait_recv()
        qs[t] = (qay[t, block(lo, 128), :].astype(F32) + qx[t].astype(F32)).astype(BF16)
        for c in q1_copies(t):
            c.start()
        for k, c in enumerate(y1_copies(t)):
            c.wait_recv()
            rows = block(2 * (yp, ym)[k] + k, 32)
            pay[t, rows, :] = (pay[t, rows, :].astype(F32) + y1[t, k].astype(F32)).astype(BF16)
        for c in y2_copies(t):
            c.start()

    def after_2(t):
        for k, c in enumerate(q1_copies(t)):
            c.wait_recv()
            rows = block(2 * (yp, ym)[k] + k, 16)
            qs[t, rows, :] = (qs[t, rows, :].astype(F32) + q1[t, k].astype(F32)).astype(BF16)
        for c in q2_copies(t):
            c.start()
        for c in y2_copies(t):
            c.wait_recv()
        total = pay[t, block(y, 64), :].astype(F32) + y2[t, 0].astype(F32) + y2[t, 1].astype(F32)
        zs[t] = total.astype(BF16)
        z_send(t)

    def after_3(t):
        for c in q2_copies(t):
            c.wait_recv()
        total = qs[t, block(y, 32), :].astype(F32) + q2[t, 0].astype(F32) + q2[t, 1].astype(F32)
        qz[t] = total.astype(BF16)
        qz_send(t)
        z_all(t).wait_recv()
        total = zs[t, :, block(z, 128)].astype(F32)
        for d in range(7):
            total = total + zr[t, d].astype(F32)
        xk[t] = total
        xs[t] = xk[t, block(1 - lo, 32), :].astype(BF16)
        x_copy(t).start()

    def after_4(t):
        is_b, is_h, g = round_of(t)
        slot = is_b + 2 * is_h
        row = g + is_h * core * 2
        x_copy(t).wait_recv()
        total = xk[t, block(lo, 32), :] + xr[t].astype(F32)
        fin[slot, block(row, 32), :] = total.astype(BF16)
        qz_all(t).wait_recv()
        total = qz[t, :, block(z, 128)].astype(F32)
        for d in range(7):
            total = total + qr[t, d].astype(F32)
        fin[slot, block(row + 1, 32), :] = total.astype(BF16)

    zero = jnp.zeros((128, 128), BF16)
    fin[2] = zero

    def step(t, carry):
        @pl.when(t == 3)
        def _():
            vec[0] = vec_sum(0, vec.at[2])
            vec_send(1, vec.at[0])

        @pl.when(t == 6)
        def _():
            vec[1] = vec_sum(1, vec.at[0])
            vec_send(2, vec.at[1])

        for lag, work in ((8, after_4), (6, after_3), (4, after_2), (2, after_1), (0, compute)):

            @pl.when((t >= lag) & (t < ROUNDS + lag))
            def _(lag=lag, work=work):
                work(t - lag)

        return carry

    lax.fori_loop(0, ROUNDS + 8, step, 0)

    fint[0] = fin[1].astype(F32).T.astype(BF16)
    fint[1] = fin[2].astype(F32).T.astype(BF16)

    direct = block(z, 128)
    mirror = block(2 * y + lo, 128)
    half = block(core, 64)
    pieces = [fin.at[0, pl.ds(64 * e, 64)] for e in range(2)] + [fin.at[1, pl.ds(64 * e, 64)] for e in range(2)]
    pieces += [fint.at[0, pl.ds(64 * e, 64)] for e in range(2)]
    pieces += [fin.at[2, half]] + [fint.at[1, pl.ds(64 * e, 64)] for e in range(2)]
    places = [own.at[0, :, direct]] * 4 + [own.at[0, :, mirror]] * 2 + [own.at[0, :, direct]] + [own.at[core, :, mirror]] * 2
    sems = [own_sem.at[0]] * 7 + [own_sem.at[core]] * 2
    sends = list(zip(pieces, places, sems, holders))

    for k, (src, dst, sem, to) in enumerate(sends):

        @pl.when(flat(to) != me)
        def _(k=k, src=src, dst=dst, sem=sem, to=to):
            remote(src, dst, f_s.at[k], sem, to).start()

        @pl.when(flat(to) == me)
        def _(src=src, dst=dst, sem=sem):
            pltpu.make_async_copy(src, dst, sem).start()

    for c in pm_copies:
        c.wait_recv()
    resid = t_row - (pmv[...] + pmr[0] + pmr[1] + pmr[2])
    resid = resid * resid
    total = sum(resid[:, 128 * j : 128 * j + 128] for j in range(count // 128))
    total = jnp.broadcast_to(total / 32, (8, 128)) - square[...]
    pltpu.make_async_copy(covb, covb, cov_r).wait()
    for k, piece in enumerate(pieces):
        total = total + jnp.sum((covb[k] * piece[...].astype(F32)).reshape(8, 8, 128), axis=0)
    vec[3] = total
    vec_send(3, vec.at[3])
    per_noise = 0.5 / hypers[1]
    nat_out[...] = 0.5 * nat[...] + vec_sum(2, vec.at[1]) * per_noise
    vec[4] = vec_sum(3, vec.at[3])
    vec_send(4, vec.at[4])

    pltpu.make_async_copy(own.at[0], own.at[0], own_sem.at[0]).wait()

    @pl.when(both == 1)
    def _():
        pltpu.make_async_copy(own.at[1], own.at[1], own_sem.at[1]).wait()
        own[0] = own[0] + own[1]

    gap = ((z * 2 + lo) * 4 + y) * 64 - mine * 1024
    for i in range(8):
        rows = slice(8 * i, 8 * i + 8)
        shape = (8, 1024)
        same = lax.broadcasted_iota(jnp.int32, shape, 1) - lax.broadcasted_iota(jnp.int32, shape, 0) == gap + 8 * i
        out[rows] = 0.5 * prec[rows] + (jnp.where(same, 0.5, 0.0) + own[0, rows].astype(F32) * per_noise)

    points = 64.0 * count
    total = jnp.sum(vec_sum(4, vec.at[4]), axis=(0, 1), keepdims=True) + hypers[0] * points
    noise = jnp.full((1, 1), hypers[1], F32)
    fit_out[...] = -0.5 * jnp.log(2.0 * jnp.pi * noise) - total / (2.0 * noise * points)
    for k in range(5):
        into = vec_into(k)
        remote(into, into, v_s.at[k], v_r.at[k], partner).wait_send()
    cov_sends(0, cov_sent)

    @pl.when(both == 1)
    def _():
        cov_sends(1, cov_sent)

    for k, (src, dst, sem, to) in enumerate(sends):

        @pl.when(flat(to) != me)
        def _(k=k, src=src, dst=dst, sem=sem, to=to):
            remote(src, dst, f_s.at[k], sem, to).wait_send()

    for c in pm_copies:
        c.wait_send()
    for c in (over, near, on, to_partner):
        c.wait_send()

    def drain(t, carry):
        for c in y1_copies(t) + y2_copies(t) + q1_copies(t) + q2_copies(t):
            c.wait_send()
        for c in (z_all(t), x_copy(t), qz_all(t), qx_copy(t)):
            c.wait_send()
        return carry

    lax.fori_loop(0, ROUNDS, drain, 0)
    lax.fori_loop(0, 4, lambda g, c: (gather_all(g).wait_send(), c)[1], 0)


def step(hypers, ind_t, pts, tgt, scale, mean, whitening, cov, prec, nat):
    dma = pltpu.SemaphoreType.DMA
    n = pts.shape[1]
    return pl.pallas_call(
        kernel,
        out_shape=tuple(jax.ShapeDtypeStruct(s, F32) for s in ((64, 1024), (8, 128), (1, 1))),
        in_specs=[pl.BlockSpec(memory_space=pltpu.SMEM)] + [VMEM] * 5 + [ANY] + [VMEM] * 3,
        out_specs=(VMEM, VMEM, VMEM),
        scratch_shapes=[
            pltpu.VMEM((4, 64, 1024), F32),
            pltpu.VMEM((64, n), BF16),
            pltpu.VMEM(tgt.shape, F32),
            pltpu.VMEM((2, 1024, 2048), BF16),
            pltpu.VMEM((2, 2048, n), BF16),
            pltpu.VMEM((1024, n), F32),
            pltpu.VMEM((8, 128), F32),
            pltpu.VMEM((1, n), F32),
            pltpu.VMEM((9, 64, 128), F32),
            pltpu.VMEM((3, 1024, n), BF16),
            pltpu.VMEM((ROUNDS, 256, 1024), BF16),
            pltpu.VMEM((ROUNDS, 2, 32, 1024), BF16),
            pltpu.VMEM((ROUNDS, 2, 64, 1024), BF16),
            pltpu.VMEM((ROUNDS, 64, 1024), BF16),
            pltpu.VMEM((ROUNDS, 7, 64, 128), BF16),
            pltpu.VMEM((ROUNDS, 64, 128), F32),
            pltpu.VMEM((ROUNDS, 32, 128), BF16),
            pltpu.VMEM((ROUNDS, 32, 128), BF16),
            pltpu.VMEM((ROUNDS, 256, 1024), BF16),
            pltpu.VMEM((ROUNDS, 128, 1024), BF16),
            pltpu.VMEM((ROUNDS, 128, 1024), BF16),
            pltpu.VMEM((ROUNDS, 2, 16, 1024), BF16),
            pltpu.VMEM((ROUNDS, 2, 32, 1024), BF16),
            pltpu.VMEM((ROUNDS, 32, 1024), BF16),
            pltpu.VMEM((ROUNDS, 7, 32, 128), BF16),
            pltpu.VMEM((3, 128, 128), BF16),
            pltpu.VMEM((2, 128, 128), BF16),
            pltpu.VMEM((2, 64, 1024), BF16),
            pltpu.VMEM((3, 1, n), F32),
            pltpu.VMEM((5, 8, 128), F32),
            pltpu.VMEM((3, 8, 128), F32),
            pltpu.VMEM((7, 8, 128), F32),
            pltpu.VMEM((1, 8, 128), F32),
            pltpu.VMEM((15, 8, 128), F32),
            pltpu.VMEM((15, 8, 128), F32),
            dma((5,)), dma((5,)), dma((3,)), dma((16,)), dma,
            dma((4,)), dma((4,)), dma, dma,
            dma((ROUNDS, 2)), dma((ROUNDS, 2)), dma((ROUNDS, 2)), dma((ROUNDS, 2)),
            dma((ROUNDS,)), dma((ROUNDS,)), dma((ROUNDS,)), dma((ROUNDS,)),
            dma((ROUNDS,)), dma((ROUNDS,)), dma((ROUNDS, 2)), dma((ROUNDS, 2)),
            dma((ROUNDS, 2)), dma((ROUNDS, 2)), dma((ROUNDS,)), dma((ROUNDS,)),
            dma((3,)), dma((3,)), dma((9,)), dma((2,)), dma((5,)), dma((5,)),
        ],
        compiler_params=pltpu.CompilerParams(has_side_effects=True, collective_id=0, vmem_limit_bytes=56 * 2**20),
        name="gp_step",
    )(hypers, ind_t, pts, tgt, scale, mean, whitening, cov, prec, nat)


def shards(points, targets, inducing, whitening, mean_v, covariance, precision, natural_one, lengthscales, hypers):
    own_rows, own_points = inducing.shape[0], points.shape[0]
    precision_new, natural_new, expected_fit = step(
        hypers,
        inducing.T,
        points.T,
        targets.reshape(own_points // 128, 128),
        lengthscales.reshape(1, -1),
        mean_v.reshape(8, 128),
        whitening,
        covariance.T,
        precision.T,
        natural_one.reshape(8, 128),
    )
    return precision_new.T, natural_new.reshape(own_rows), expected_fit.reshape(())


def solution(mesh):
    finer = Mesh(mesh.devices.reshape(8, 2, mesh.shape["rep"], 2, 2), AXES)
    return jax.shard_map(
        shards,
        mesh=finer,
        in_specs=(
            P(DP_REP, None), P(DP_REP), P(IND, None), P(IND, None), P(IND),
            P(IND, DP_REP), P(IND, DP_REP), P(IND), P(), P(),
        ),
        out_specs=(P(IND, DP_REP), P(IND), P()),
        check_vma=False,
    )
```

```python
import jax
import jax.numpy as jnp
from jax import lax
from jax.experimental import pallas as pl
from jax.experimental.pallas import tpu as pltpu
from jax.sharding import Mesh
from jax.sharding import PartitionSpec as P

AXES = ("dp_0", "dp_1", "rep", "ind_0", "ind_1")
IND = ("ind_0", "ind_1")
DP_REP = ("dp_0", "dp_1", "rep")
MESH = pl.DeviceIdType.MESH
VMEM = pl.BlockSpec(memory_space=pltpu.VMEM)
ANY = pl.BlockSpec(memory_space=pl.ANY)
F32 = jnp.float32
BF16 = jnp.bfloat16
ROUNDS = 5
TALL = (32, 32, 32, 48, 16)
PIECES = ((0, 32), (32, 48), (80, 32), (112, 16))


def place():
    return tuple(lax.axis_index(a) for a in AXES)


def remote(src, dst, send, recv, to):
    return pltpu.make_async_remote_copy(
        src_ref=src, dst_ref=dst, send_sem=send, recv_sem=recv, device_id=to, device_id_type=MESH
    )


def parts_of(v):
    a = v.astype(BF16)
    b = (v - a.astype(F32)).astype(BF16)
    return a, b, (v - a.astype(F32) - b.astype(F32)).astype(BF16)


def tile_of(v):
    row = lax.broadcasted_iota(jnp.int32, (16, v.shape[1]), 0)
    tile = jnp.zeros((16, v.shape[1]), F32)
    for k, part in enumerate(parts_of(v)):
        tile = jnp.where(row == k, part.astype(F32), tile)
    return tile.astype(BF16)


def dot(a, b, dims):
    return lax.dot_general(a, b, ((dims[:1], dims[1:]), ((), ())), preferred_element_type=F32)


def round_of(t):
    is_b = t // 3
    is_h = (t // 2) * (1 - is_b)
    g = 2 * ((t + is_b) % 2) * (1 - is_h)
    return is_b, is_h, g


def kernel(
    hypers, ind_t, pts_in, tgt_in, scale_in, mean, whitening, cov, prec, nat, out, nat_out, fit_out,
    zall, pts, tgt, wv, cross, acc, square, pmv, covb,
    wbuf, pay, y1, y2, zs, zr, xk, xs, xr, qay, qx, qs, q1, q2, qz, qr, fin, fint, own, pmr, vec, vy, vz, vx, va, vb,
    i_s, i_r, c_s, cov_s, cov_r,
    g_s, g_r, p_s, p_r, y1_s, y1_r, y2_s, y2_r, z_s, z_r, x_s, x_r,
    qx_s, qx_r, q1_s, q1_r, q2_s, q2_r, qz_s, qz_r, dz_s, dz_r, dq_s, pm_s, pm_r, f_s, own_sem, v_s, v_r,
):
    z, lo, y, hi, core = place()
    mine = hi * 2 + core
    yp, ym, y2p = (y + 1) % 4, (y + 3) % 4, (y + 2) % 4
    partner = (z, lo, y, hi, 1 - core)
    gather_to = (z, 1 - lo, y, 1 - hi, (core + 1 - hi) % 2)

    count = pts.shape[1]
    cut = wv.shape[2]
    w_copies = [
        pltpu.make_async_copy(
            whitening.at[:, pl.ds(pl.multiple_of((hi + h - 2 * hi * h) * cut, cut), cut)], wv.at[h], c_s.at[h]
        )
        for h in range(2)
    ]
    for c in w_copies:
        c.start()
    line = [
        (z, (lo + d // 4) % 2, y, (hi + (d // 2) % 2) % 2, (core + d % 2) % 2) for d in range(1, 8)
    ]
    over_y = [(z, lo, (y + d) % 4, hi, core) for d in range(1, 4)]
    over_z = [((z + d) % 8, lo, y, hi, core) for d in range(1, 8)]
    low, high = hi * 2, hi * 2 + 1
    nxt = (1 - hi) * 2 + (core + hi) % 2
    prv = (1 - hi) * 2 + (core + 1 - hi) % 2

    def owner(q, ind):
        return (q // 8, (q // 4) % 2, q % 4, ind // 2, ind % 2)

    def flat(d):
        return (((d[0] * 2 + d[1]) * 4 + d[2]) * 2 + d[3]) * 2 + d[4]

    def equal(a, b):
        return 1 - jnp.minimum(jnp.abs(a - b), 1)

    me = flat(place())
    here = 4 * y + 2 * lo
    holders = (
        [owner(16 * mine + here + e, mine) for e in range(2)]
        + [owner(16 * nxt + here + e, mine) for e in range(2)]
        + [owner(16 * mine + 2 * z + e, nxt) for e in range(2)]
        + [owner(16 * high + here + core, low)]
        + [owner(16 * low + 2 * z + e, high) for e in range(2)]
        + [owner(16 * mine + 2 * z + e, mine) for e in range(2)]
    )

    def ahead(half):
        return (z - 2 * y - half + 8) % 8

    def formed(half):
        return 1 - jnp.minimum(ahead(half) // 5, 1)

    alone = equal(ahead(lo), 0) + jnp.minimum(ahead(lo) // 4, 1)
    needed = [formed(lo)] * 2 + [1] * 7 + [1 - alone] * 2
    own_group, own_q = z // 2, (z % 2) * 8 + lo * 4 + y
    is_d, is_n, is_p = equal(own_group, mine), equal(own_group, nxt), equal(own_group, prv)
    is_s = 1 - is_d - is_n - is_p
    both = is_s * core

    def cov_target(i, second):
        e = own_q % 2
        far = is_d * jnp.minimum((i - own_q // 2 + 8) % 8 // 5, 1)
        mirrored = is_p + is_s * core + far
        to_core = is_p * (own_group % 2) + is_s * ((1 - core) * e + core * second) + (1 - is_p - is_s) * core
        to = (
            (1 - mirrored) * i + mirrored * (own_q // 2),
            (1 - mirrored) * ((own_q // 2) % 2) + mirrored * (i % 2),
            (1 - mirrored) * (own_q // 4) + mirrored * (i // 2),
            is_p * (own_group // 2) + (1 - is_p) * hi,
            to_core,
        )
        slot = is_d * e + far * 9 + is_n * (2 + e) + is_p * (4 + e) + is_s * ((1 - core) * 6 + core * (7 + e))
        return to, cov.at[:, pl.ds(pl.multiple_of(i * 128, 128), 128)], covb.at[slot], cov_r.at[is_d + far]

    covb[...] = jnp.zeros(covb.shape, F32)
    fin[...] = jnp.zeros(fin.shape, BF16)
    barrier = pltpu.get_barrier_semaphore()
    arrivals = 17 + 8 * (1 + both)
    for to in over_y + over_z + line:
        pl.semaphore_signal(barrier, inc=1, device_id=to, device_id_type=MESH)
    for to, need in zip(holders, needed):
        arrivals = arrivals - need * equal(flat(to), me)

        @pl.when(need * (1 - equal(flat(to), me)) == 1)
        def _(to=to):
            pl.semaphore_signal(barrier, inc=1, device_id=to, device_id_type=MESH)

    pl.semaphore_wait(barrier, arrivals)

    over_a = [((z + d) % 8, lo, y, hi, (core + c) % 2) for d in range(8) for c in range(2) if d + c]
    over_b = [
        (z, (lo + a) % 2, (y + d) % 4, (hi + b) % 2, core)
        for d in range(4)
        for a in range(2)
        for b in range(2)
        if d + a + b
    ]

    def cov_sends(second, act):
        def one(i, carry):
            to, src, dst, sem = cov_target(i, second)

            @pl.when(flat(to) != me)
            def _():
                act(remote(src, dst, cov_s.at[8 * second + i], sem, to), True)

            @pl.when(flat(to) == me)
            def _():
                act(pltpu.make_async_copy(src, dst, sem), False)

            return carry

        lax.fori_loop(0, 8, one, 0)

    def cov_start(copy, far):
        copy.start()

    def cov_sent(copy, far):
        if far:
            copy.wait_send()

    def vec_into(k):
        return (vy, vz, vx, va, vb)[k]

    def vec_send(k, src):
        for i, to in enumerate((over_y, over_z, [(z, 1 - lo, y, hi, core)], over_a, over_b)[k]):
            remote(src, vec_into(k).at[i], v_s.at[k], v_r.at[k], to).start()

    def vec_sum(k, src):
        into = vec_into(k)
        remote(into, into, v_s.at[k], v_r.at[k], partner).wait_recv()
        total = src[...]
        return total + sum(into[i] for i in range(into.shape[0]))

    other = (1 - hi) * 2 + core
    across = (z, 1 - lo, y, 1 - hi, core)
    swap = (z, 1 - lo, y, hi, core)
    over = remote(ind_t, zall.at[mine], i_s.at[0], i_r.at[0], across)
    near = remote(ind_t, zall.at[mine], i_s.at[1], i_r.at[1], partner)
    on = remote(zall.at[other], zall.at[other], i_s.at[2], i_r.at[2], partner)
    swaps = (
        remote(pts_in, pts, i_s.at[3], i_r.at[3], swap),
        remote(tgt_in, tgt, i_s.at[4], i_r.at[4], swap),
    )

    @pl.when(hi == 0)
    def _():
        for c in swaps:
            c.start()

    over.start()
    near.start()
    own_z = pltpu.make_async_copy(ind_t, zall.at[mine], c_s.at[2])
    own_z.start()

    @pl.when(hi == 1)
    def _():
        pts[...] = pts_in[...]
        tgt[...] = tgt_in[...]

    own_z.wait()

    @pl.when(hi == 0)
    def _():
        for c in swaps:
            c.wait()

    diagonal = lax.broadcasted_iota(jnp.int32, (64, 64), 0) == lax.broadcasted_iota(jnp.int32, (64, 64), 1)
    scale = jnp.sum(jnp.where(diagonal, jnp.broadcast_to(scale_in[...], (64, 64)), 0.0), axis=1, keepdims=True)
    scales = jnp.broadcast_to(scale, (64, count))
    t_row = jnp.concatenate([tgt[j : j + 1, :] for j in range(count // 128)], axis=1)
    norm_x = 0.5 * jnp.sum(jnp.square(pts[...].astype(F32) / scales), axis=0, keepdims=True)
    three = lax.broadcasted_iota(jnp.int32, (16, count), 0) < 3
    p_mat = jnp.concatenate([pts[...]] * 3 + [jnp.where(three, 1.0, 0.0).astype(BF16)], axis=0)

    def cross_rows(held, half, at):
        def piece(j, carry):
            cols = pl.ds(pl.multiple_of(j * 256, 256), 256)
            zt = zall[held, :, cols]
            s = jnp.broadcast_to(scale, (64, 256))
            zs_ = zt / s
            norm = tile_of(-0.5 * jnp.sum(zs_ * zs_, axis=0, keepdims=True))
            z_mat = jnp.concatenate([*parts_of(zs_ / s), norm], axis=0)
            power = dot(z_mat, p_mat, (0, 0)) - norm_x
            rows = pl.ds(pl.multiple_of(at * 1024 + j * 256, 256), 256)
            cross[half, rows, :] = (hypers[0] * jnp.exp(power)).astype(BF16)
            return carry

        lax.fori_loop(0, 4, piece, 0)

    cross_rows(mine, 0, core)
    near.wait_recv()
    cross_rows(hi * 2 + 1 - core, 0, 1 - core)
    w_copies[0].wait()

    def first_half(i, carry):
        rows = pl.ds(pl.multiple_of(i * 256, 256), 256)
        for j in range(count // 256):
            cols = slice(256 * j, 256 * j + 256)
            acc[rows, cols] = dot(wv[0, rows, :], cross[0, :, cols], (1, 0))
        return carry

    lax.fori_loop(0, 3, first_half, 0)
    over.wait_recv()
    on.start()
    cov_sends(0, cov_start)

    @pl.when(both == 1)
    def _():
        cov_sends(1, cov_start)

    lax.fori_loop(3, 4, first_half, 0)
    cross_rows(other, 1, core)
    on.wait_recv()
    cross_rows((1 - hi) * 2 + 1 - core, 1, 1 - core)
    w_copies[1].wait()
    square[...] = jnp.zeros((8, 128), F32)

    def gather_start(c):
        first, size = PIECES[c]

        def one(k, carry):
            rows = pl.ds(pl.multiple_of(k * 128 + first, 16), size)
            remote(wbuf.at[core, rows], wbuf.at[2, rows], g_s.at[c], g_r.at[c], gather_to).start()
            return carry

        lax.fori_loop(0, 8, one, 0)

    def second_half(g, carry):
        rows = [pl.ds(pl.multiple_of(k * 128 + 32 * g, 32), 32) for k in range(8)]
        a = jnp.concatenate([wv[1, r, :] for r in rows], axis=0)
        for j in range(count // 256):
            cols = slice(256 * j, 256 * j + 256)
            part = dot(a, cross[1, :, cols], (1, 0)) + jnp.concatenate([acc[r, cols] for r in rows], axis=0)
            part = part.astype(BF16)
            for k, r in enumerate(rows):
                wbuf[core, r, cols] = part[32 * k : 32 * k + 32]
            wide = part.astype(F32)
            both = jnp.sum((wide * wide).reshape(32, 8, 256), axis=0)
            square[...] += both[:, :128] + both[:, 128:]
        for c, done in enumerate((0, 2, 3, 3)):

            @pl.when(g == done)
            def _(c=c):
                gather_start(c)

        return carry

    lax.fori_loop(0, 4, second_half, 0)
    to_partner = remote(wbuf.at[core], wbuf.at[core], p_s, p_r, partner)
    to_partner.start()
    def gather_all(g):
        rows = pl.ds(0, 8 * PIECES[g][1])
        return remote(wbuf.at[core, rows], wbuf.at[2, rows], g_s.at[g], g_r.at[g], gather_to)

    up_y, down_y = (z, lo, yp, hi, core), (z, lo, ym, hi, core)
    over_x = (z, 1 - lo, y, hi, core)

    def block(k, size):
        return pl.ds(pl.multiple_of(k * size, size), size)

    def wide(t):
        return pl.ds(0, 640 if t < 2 else 1024)

    def y1_copies(t):
        h, w = TALL[t], wide(t)
        return tuple(
            remote(pay.at[t, block(2 * y2p + k, h), w], y1.at[t, k, pl.ds(0, h), w], y1_s.at[t, k], y1_r.at[t, k], to)
            for k, to in enumerate((up_y, down_y))
        )

    def y2_copies(t):
        h, w = 2 * TALL[t], wide(t)
        return tuple(
            remote(pay.at[t, block(at, h), w], y2.at[t, k, pl.ds(0, h), w], y2_s.at[t, k], y2_r.at[t, k], to)
            for k, (at, to) in enumerate(((yp, up_y), (ym, down_y)))
        )

    def d_copies(t, second):
        halves = (lo,) if second else (0, 1)
        out = []
        for h, half in enumerate(halves):
            for d in range(5):
                to = (2 * y + half + d) % 8
                slot = (to - z + 7) % 8
                cols = slice(128 * d, 128 * d + 128)
                if second:
                    c = (qz.at[t, :, cols], qr.at[t, slot], dq_s.at[t, d], qz_r.at[t])
                else:
                    rows = pl.ds(32 * h, 32)
                    c = (zs.at[t, rows, cols], zr.at[t, slot, rows], dz_s.at[t, 5 * h + d], dz_r.at[t, h])
                out.append((to, c))
        return out

    def d_act(t, second, act):
        for to, c in d_copies(t, second):

            @pl.when(to != z)
            def _(to=to, c=c):
                act(remote(*c, (to, lo, y, hi, core)))

    def z_send(t):
        if t < 2:
            d_act(t, 0, lambda c: c.start())
            return
        for d in range(1, 8):
            to = (z + d) % 8
            rows = pl.ds(0, 2 * TALL[t])
            remote(zs.at[t, rows, block(to, 128)], zr.at[t, d - 1, rows], z_s.at[t], z_r.at[t], over_z[d - 1]).start()

    def z_all(t):
        part = zr.at[t, :, pl.ds(0, 2 * TALL[t])]
        return remote(part, part, z_s.at[t], z_r.at[t], over_x)

    def x_copy(t):
        rows = pl.ds(0, TALL[t])
        return remote(xs.at[t, rows], xr.at[t, rows], x_s.at[t], x_r.at[t], over_x)

    def qx_copy(t):
        return remote(qay.at[t, block(1 - lo, 128), wide(t)], qx.at[t, :, wide(t)], qx_s.at[t], qx_r.at[t], over_x)

    def q1_copies(t):
        return (
            remote(qs.at[t, block(2 * y2p, 16), wide(t)], q1.at[t, 0, :, wide(t)], q1_s.at[t, 0], q1_r.at[t, 0], up_y),
            remote(qs.at[t, block(2 * y2p + 1, 16), wide(t)], q1.at[t, 1, :, wide(t)], q1_s.at[t, 1], q1_r.at[t, 1], down_y),
        )

    def q2_copies(t):
        return (
            remote(qs.at[t, block(yp, 32), wide(t)], q2.at[t, 0, :, wide(t)], q2_s.at[t, 0], q2_r.at[t, 0], up_y),
            remote(qs.at[t, block(ym, 32), wide(t)], q2.at[t, 1, :, wide(t)], q2_s.at[t, 1], q2_r.at[t, 1], down_y),
        )

    def qz_send(t):
        if t < 2:
            d_act(t, 1, lambda c: c.start())
            return
        for d in range(1, 8):
            to = (z + d) % 8
            remote(qz.at[t, :, block(to, 128)], qr.at[t, d - 1], qz_s.at[t], qz_r.at[t], over_z[d - 1]).start()

    def qz_all(t):
        return remote(qr.at[t], qr.at[t], qz_s.at[t], qz_r.at[t], over_x)

    def slab(t, first, h, groups, into):
        is_b, is_h, _ = round_of(t)
        plain = 1 - is_h
        left = is_b * 2 + is_h + plain * (1 - is_b) * core
        right = plain * core
        first = first + is_h * 64 * core
        a = jnp.concatenate([wbuf[left, pl.ds(pl.multiple_of(k * 128 + first, 16), h), :] for k in groups], axis=0)
        for j in range(4):
            b = wbuf[right, j * 256 : (j + 1) * 256, :]
            part = dot(a, b, (1, 1)).astype(BF16)
            if t > 1:
                into[t, : 8 * h, j * 256 : (j + 1) * 256] = part
                continue
            for r, k in enumerate(groups):
                for h in range(2):
                    d = (2 * j + h - k) % 8
                    if d < 5:
                        into[t, 32 * r : 32 * r + 32, 128 * d : 128 * d + 128] = part[
                            32 * r : 32 * r + 32, 128 * h : 128 * h + 128
                        ]

    def qx_start(t):
        is_b, is_h, g = round_of(t)

        if t == 2:
            to_partner.wait_recv()
        if t > 2:
            gather_all(g).wait_recv()
        slab(t, PIECES[g][0] if t > 2 else 32 * g, 32, (0, 2, 4, 6, 1, 3, 5, 7), qay)
        qx_copy(t).start()

    def y1_start(t):
        is_b, is_h, g = round_of(t)

        if t > 2:
            gather_all(g + 1).wait_recv()
        slab(t, PIECES[g + 1][0] if t > 2 else 32 * (g + 1), TALL[t], range(8), pay)
        for c in y1_copies(t):
            c.start()

    def after_qx(t):
        qx_copy(t).wait_recv()
        w = wide(t)
        qs[t, :, w] = (qay[t, block(lo, 128), w].astype(F32) + qx[t, :, w].astype(F32)).astype(BF16)
        for c in q1_copies(t):
            c.start()

    def after_y1(t):
        for k, c in enumerate(y1_copies(t)):
            c.wait_recv()
            h, w = TALL[t], wide(t)
            rows = block(2 * (yp, ym)[k] + k, h)
            pay[t, rows, w] = (pay[t, rows, w].astype(F32) + y1[t, k, :h, w].astype(F32)).astype(BF16)
        for c in y2_copies(t):
            c.start()

    def after_q1(t):
        for k, c in enumerate(q1_copies(t)):
            c.wait_recv()
            rows = block(2 * (yp, ym)[k] + k, 16)
            w = wide(t)
            qs[t, rows, w] = (qs[t, rows, w].astype(F32) + q1[t, k, :, w].astype(F32)).astype(BF16)
        for c in q2_copies(t):
            c.start()

    def after_y2(t):
        for c in y2_copies(t):
            c.wait_recv()
        h, w = 2 * TALL[t], wide(t)
        total = pay[t, block(y, h), w].astype(F32) + y2[t, 0, :h, w].astype(F32) + y2[t, 1, :h, w].astype(F32)
        zs[t, :h, w] = total.astype(BF16)
        z_send(t)

    def after_q2(t):
        for c in q2_copies(t):
            c.wait_recv()
        w = wide(t)
        total = qs[t, block(y, 32), w].astype(F32) + q2[t, 0, :, w].astype(F32) + q2[t, 1, :, w].astype(F32)
        qz[t, :, w] = total.astype(BF16)
        qz_send(t)

    def after_z(t):
        if t < 2:
            for h in range(2):
                rows = pl.ds(32 * h, 32)

                @pl.when(formed(h) == 1)
                def _(h=h, rows=rows):
                    remote(zr.at[t, :, rows], zr.at[t, :, rows], x_s.at[t], dz_r.at[t, h], over_x).wait_recv()
                    total = zs[t, rows, block(jnp.minimum(ahead(h), 4), 128)].astype(F32)
                    xk[t, rows, :] = total + sum(zr[t, d, rows].astype(F32) for d in range(7))

            @pl.when(formed(1 - lo) == 1)
            def _():
                xs[t, :32] = xk[t, block(1 - lo, 32), :].astype(BF16)
                x_copy(t).start()

            return
        z_all(t).wait_recv()
        h = TALL[t]
        total = zs[t, : 2 * h, block(z, 128)].astype(F32)
        for d in range(7):
            total = total + zr[t, d, : 2 * h].astype(F32)
        xk[t, : 2 * h] = total
        xs[t, :h] = xk[t, block(1 - lo, h), :].astype(BF16)
        x_copy(t).start()

    def finish(t, second, total):
        is_b, is_h, g = round_of(t)
        first = PIECES[g + second][0] if t > 2 else 32 * (g + second)
        rows = pl.ds(pl.multiple_of(first + is_h * core * 64, 16), total.shape[0])
        fin[is_b + 2 * is_h, rows, :] = total.astype(BF16)

    def after_qz(t):
        if t < 2:

            @pl.when(formed(lo) == 1)
            def _():
                qz_all(t).wait_recv()
                total = qz[t, :, block(jnp.minimum(ahead(lo), 4), 128)].astype(F32)
                finish(t, 0, total + sum(qr[t, d].astype(F32) for d in range(7)))

            return
        qz_all(t).wait_recv()
        total = qz[t, :, block(z, 128)].astype(F32)
        for d in range(7):
            total = total + qr[t, d].astype(F32)
        finish(t, 0, total)

    def after_x(t):
        def add():
            x_copy(t).wait_recv()
            h = TALL[t]
            finish(t, 1, xk[t, block(lo, h), :] + xr[t, :h].astype(F32))

        if t < 2:
            pl.when(formed(lo) == 1)(add)
        else:
            add()

    pm_to = (partner, (z, 1 - lo, y, 1 - hi, core), (z, 1 - lo, y, 1 - hi, 1 - core))
    pm_copies = [remote(pmv, pmr.at[k], pm_s.at[k], pm_r.at[k], to) for k, to in enumerate(pm_to)]

    def means_and_proj():
        m_row = jnp.concatenate([mean[j : j + 1, :] for j in range(8)], axis=1)
        pmv[...] = jnp.sum(dot(tile_of(m_row), wbuf[core], (1, 0)), axis=0, keepdims=True)
        for c in pm_copies:
            c.start()
        proj = jnp.sum(dot(tile_of(t_row), wbuf[core], (1, 1)), axis=0, keepdims=True)
        vec[2] = jnp.concatenate([proj[:, 128 * j : 128 * j + 128] for j in range(8)], axis=0)
        vec_send(0, vec.at[2])

    direct = block(z, 128)
    mirror = block(2 * y + lo, 128)
    half = block(core, 64)
    pieces = [fin.at[0, pl.ds(64 * e, 64)] for e in range(2)] + [fin.at[1, pl.ds(64 * e, 64)] for e in range(2)]
    pieces += [fint.at[0, pl.ds(64 * e, 64)] for e in range(2)]
    pieces += [fin.at[2, half]] + [fint.at[1, pl.ds(64 * e, 64)] for e in range(2)]
    pieces += [fint.at[2, pl.ds(64 * e, 64)] for e in range(2)]
    places = [own.at[0, :, direct]] * 4 + [own.at[0, :, mirror]] * 2 + [own.at[0, :, direct]] + [own.at[core, :, mirror]] * 2
    places += [own.at[0, :, mirror]] * 2
    sems = [own_sem.at[0]] * 7 + [own_sem.at[core]] * 2 + [own_sem.at[0]] * 2
    sends = list(zip(pieces, places, sems, holders))

    def deliver(some):
        for k in some:
            src, dst, sem, to = sends[k]

            @pl.when(needed[k] * (1 - equal(flat(to), me)) == 1)
            def _(k=k, src=src, dst=dst, sem=sem, to=to):
                remote(src, dst, f_s.at[k], sem, to).start()

            @pl.when(needed[k] * equal(flat(to), me) == 1)
            def _(src=src, dst=dst, sem=sem):
                pltpu.make_async_copy(src, dst, sem).start()

        return sum(
            jnp.sum((covb[k] * pieces[k][...].astype(F32)).reshape(8, 8, 128), axis=0) for k in some
        )

    def early():
        for c in pm_copies:
            c.wait_recv()
        resid = t_row - (pmv[...] + pmr[0] + pmr[1] + pmr[2])
        resid = resid * resid
        total = sum(resid[:, 128 * j : 128 * j + 128] for j in range(count // 128))
        total = jnp.broadcast_to(total / 32, (8, 128)) - square[...]
        fint[1] = fin[2].astype(F32).T.astype(BF16)
        fint[2] = fin[0].astype(F32).T.astype(BF16)
        for k, first, last in ((0, 2, 9), (1, 0, 2), (2, 9, 11)):
            some = covb.at[pl.ds(first, last - first)]

            @pl.when(needed[first] == 1)
            def _(k=k, some=some):
                pltpu.make_async_copy(some, some, cov_r.at[k]).wait()

        return total + deliver((0, 1, 6, 7, 8, 9, 10))

    order = (
        (qx_start, 0), (y1_start, 0), (qx_start, 1), (y1_start, 1), (qx_start, 2), (y1_start, 2), (qx_start, 3),
        (after_qx, 0), (after_y1, 0), (after_y1, 1), (after_y1, 2), (after_q1, 0), (after_qx, 1), (after_y2, 0),
        (after_y2, 1), (after_qx, 2), (after_y2, 2), (after_q2, 0), (after_q1, 1), (y1_start, 3), (after_z, 0),
        (after_q1, 2), (after_z, 1), (after_q2, 1), (after_qx, 3), (after_x, 0), (after_x, 1), (after_y1, 3),
        (after_z, 2), (after_q2, 2), (after_qz, 0), (after_q1, 3), (after_qz, 1), (qx_start, 4), (after_x, 2),
        (after_y2, 3), (after_qz, 2), (y1_start, 4), (after_q2, 3), (after_y1, 4), (after_qx, 4), (after_y2, 4),
        (after_q1, 4), (after_z, 3), (after_qz, 3), (after_x, 3), (after_q2, 4), (after_z, 4), (after_x, 4),
        (after_qz, 4),
    )
    for at, (work, t) in enumerate(order):
        if at == 4:
            means_and_proj()
        if at == 12:
            vec[0] = vec_sum(0, vec.at[2])
            vec_send(1, vec.at[0])
        if at == 24:
            vec[1] = vec_sum(1, vec.at[0])
            vec_send(2, vec.at[1])
        work(t)
        if at == 36:
            partial = early()

    fint[0] = fin[1].astype(F32).T.astype(BF16)
    total = partial + deliver((2, 3, 4, 5))
    vec[3] = total
    vec_send(3, vec.at[3])
    per_noise = 0.5 / hypers[1]
    nat_out[...] = 0.5 * nat[...] + vec_sum(2, vec.at[1]) * per_noise
    vec[4] = vec_sum(3, vec.at[3])
    vec_send(4, vec.at[4])

    pltpu.make_async_copy(own.at[0], own.at[0], own_sem.at[0]).wait()

    @pl.when(both == 1)
    def _():
        pltpu.make_async_copy(own.at[1], own.at[1], own_sem.at[1]).wait()
        own[0] = own[0] + own[1]

    gap = ((z * 2 + lo) * 4 + y) * 64 - mine * 1024
    for i in range(8):
        rows = slice(8 * i, 8 * i + 8)
        shape = (8, 1024)
        same = lax.broadcasted_iota(jnp.int32, shape, 1) - lax.broadcasted_iota(jnp.int32, shape, 0) == gap + 8 * i
        out[rows] = 0.5 * prec[rows] + (jnp.where(same, 0.5, 0.0) + own[0, rows].astype(F32) * per_noise)

    points = 64.0 * count
    total = jnp.sum(vec_sum(4, vec.at[4]), axis=(0, 1), keepdims=True) + hypers[0] * points
    noise = jnp.full((1, 1), hypers[1], F32)
    fit_out[...] = -0.5 * jnp.log(2.0 * jnp.pi * noise) - total / (2.0 * noise * points)
    for k in range(5):
        into = vec_into(k)
        remote(into, into, v_s.at[k], v_r.at[k], partner).wait_send()
    cov_sends(0, cov_sent)

    @pl.when(both == 1)
    def _():
        cov_sends(1, cov_sent)

    for k, (src, dst, sem, to) in enumerate(sends):

        @pl.when(needed[k] * (1 - equal(flat(to), me)) == 1)
        def _(k=k, src=src, dst=dst, sem=sem, to=to):
            remote(src, dst, f_s.at[k], sem, to).wait_send()

    for c in pm_copies:
        c.wait_send()
    for c in (over, near, on, to_partner):
        c.wait_send()

    for t in range(ROUNDS):
        for c in y1_copies(t) + y2_copies(t) + q1_copies(t) + q2_copies(t) + (qx_copy(t),):
            c.wait_send()
        if t < 2:
            d_act(t, 0, lambda c: c.wait_send())
            d_act(t, 1, lambda c: c.wait_send())
            pl.when(formed(1 - lo) == 1)(x_copy(t).wait_send)
        else:
            for c in (z_all(t), x_copy(t), qz_all(t)):
                c.wait_send()
    for c in range(4):
        gather_all(c).wait_send()


def step(hypers, ind_t, pts, tgt, scale, mean, whitening, cov, prec, nat):
    dma = pltpu.SemaphoreType.DMA
    n = pts.shape[1]
    return pl.pallas_call(
        kernel,
        out_shape=tuple(jax.ShapeDtypeStruct(s, F32) for s in ((64, 1024), (8, 128), (1, 1))),
        in_specs=[pl.BlockSpec(memory_space=pltpu.SMEM)] + [VMEM] * 5 + [ANY] + [VMEM] * 3,
        out_specs=(VMEM, VMEM, VMEM),
        scratch_shapes=[
            pltpu.VMEM((4, 64, 1024), F32),
            pltpu.VMEM((64, n), BF16),
            pltpu.VMEM(tgt.shape, F32),
            pltpu.VMEM((2, 1024, 2048), BF16),
            pltpu.VMEM((2, 2048, n), BF16),
            pltpu.VMEM((1024, n), F32),
            pltpu.VMEM((8, 128), F32),
            pltpu.VMEM((1, n), F32),
            pltpu.VMEM((11, 64, 128), F32),
            pltpu.VMEM((3, 1024, n), BF16),
            pltpu.VMEM((ROUNDS, 8 * max(TALL), 1024), BF16),
            pltpu.VMEM((ROUNDS, 2, max(TALL), 1024), BF16),
            pltpu.VMEM((ROUNDS, 2, 2 * max(TALL), 1024), BF16),
            pltpu.VMEM((ROUNDS, 2 * max(TALL), 1024), BF16),
            pltpu.VMEM((ROUNDS, 7, 2 * max(TALL), 128), BF16),
            pltpu.VMEM((ROUNDS, 2 * max(TALL), 128), F32),
            pltpu.VMEM((ROUNDS, max(TALL), 128), BF16),
            pltpu.VMEM((ROUNDS, max(TALL), 128), BF16),
            pltpu.VMEM((ROUNDS, 256, 1024), BF16),
            pltpu.VMEM((ROUNDS, 128, 1024), BF16),
            pltpu.VMEM((ROUNDS, 128, 1024), BF16),
            pltpu.VMEM((ROUNDS, 2, 16, 1024), BF16),
            pltpu.VMEM((ROUNDS, 2, 32, 1024), BF16),
            pltpu.VMEM((ROUNDS, 32, 1024), BF16),
            pltpu.VMEM((ROUNDS, 7, 32, 128), BF16),
            pltpu.VMEM((3, 128, 128), BF16),
            pltpu.VMEM((3, 128, 128), BF16),
            pltpu.VMEM((2, 64, 1024), BF16),
            pltpu.VMEM((3, 1, n), F32),
            pltpu.VMEM((5, 8, 128), F32),
            pltpu.VMEM((3, 8, 128), F32),
            pltpu.VMEM((7, 8, 128), F32),
            pltpu.VMEM((1, 8, 128), F32),
            pltpu.VMEM((15, 8, 128), F32),
            pltpu.VMEM((15, 8, 128), F32),
            dma((5,)), dma((5,)), dma((3,)), dma((16,)), dma((3,)),
            dma((4,)), dma((4,)), dma, dma,
            dma((ROUNDS, 2)), dma((ROUNDS, 2)), dma((ROUNDS, 2)), dma((ROUNDS, 2)),
            dma((ROUNDS,)), dma((ROUNDS,)), dma((ROUNDS,)), dma((ROUNDS,)),
            dma((ROUNDS,)), dma((ROUNDS,)), dma((ROUNDS, 2)), dma((ROUNDS, 2)),
            dma((ROUNDS, 2)), dma((ROUNDS, 2)), dma((ROUNDS,)), dma((ROUNDS,)),
            dma((2, 10)), dma((2, 2)), dma((2, 5)),
            dma((3,)), dma((3,)), dma((11,)), dma((2,)), dma((5,)), dma((5,)),
        ],
        compiler_params=pltpu.CompilerParams(has_side_effects=True, collective_id=0, vmem_limit_bytes=56 * 2**20),
        name="gp_step",
    )(hypers, ind_t, pts, tgt, scale, mean, whitening, cov, prec, nat)


def shards(points, targets, inducing, whitening, mean_v, covariance, precision, natural_one, lengthscales, hypers):
    own_rows, own_points = inducing.shape[0], points.shape[0]
    precision_new, natural_new, expected_fit = step(
        hypers,
        inducing.T,
        points.T,
        targets.reshape(own_points // 128, 128),
        lengthscales.reshape(1, -1),
        mean_v.reshape(8, 128),
        whitening,
        covariance.T,
        precision.T,
        natural_one.reshape(8, 128),
    )
    return precision_new.T, natural_new.reshape(own_rows), expected_fit.reshape(())


def solution(mesh):
    finer = Mesh(mesh.devices.reshape(8, 2, mesh.shape["rep"], 2, 2), AXES)
    return jax.shard_map(
        shards,
        mesh=finer,
        in_specs=(
            P(DP_REP, None), P(DP_REP), P(IND, None), P(IND, None), P(IND),
            P(IND, DP_REP), P(IND, DP_REP), P(IND), P(), P(),
        ),
        out_specs=(P(IND, DP_REP), P(IND), P()),
        check_vma=False,
    )
```

```python
import jax
import jax.numpy as jnp
from jax import lax
from jax.experimental import pallas as pl
from jax.experimental.pallas import tpu as pltpu
from jax.sharding import Mesh
from jax.sharding import PartitionSpec as P

AXES = ("dp_0", "dp_1", "rep", "ind_0", "ind_1")
IND = ("ind_0", "ind_1")
DP_REP = ("dp_0", "dp_1", "rep")
MESH = pl.DeviceIdType.MESH
VMEM = pl.BlockSpec(memory_space=pltpu.VMEM)
ANY = pl.BlockSpec(memory_space=pl.ANY)
F32 = jnp.float32
BF16 = jnp.bfloat16
ROUNDS = 5
TALL = (32, 32, 32, 48, 16)
PIECES = ((0, 32), (32, 48), (80, 32), (112, 16))


def place():
    return tuple(lax.axis_index(a) for a in AXES)


def remote(src, dst, send, recv, to):
    return pltpu.make_async_remote_copy(
        src_ref=src, dst_ref=dst, send_sem=send, recv_sem=recv, device_id=to, device_id_type=MESH
    )


def parts_of(v):
    a = v.astype(BF16)
    b = (v - a.astype(F32)).astype(BF16)
    return a, b, (v - a.astype(F32) - b.astype(F32)).astype(BF16)


def tile_of(v):
    row = lax.broadcasted_iota(jnp.int32, (16, v.shape[1]), 0)
    tile = jnp.zeros((16, v.shape[1]), F32)
    for k, part in enumerate(parts_of(v)):
        tile = jnp.where(row == k, part.astype(F32), tile)
    return tile.astype(BF16)


def dot(a, b, dims):
    return lax.dot_general(a, b, ((dims[:1], dims[1:]), ((), ())), preferred_element_type=F32)


def round_of(t):
    is_b = t // 3
    is_h = (t // 2) * (1 - is_b)
    g = 2 * ((t + is_b) % 2) * (1 - is_h)
    return is_b, is_h, g


def kernel(
    hypers, ind_t, pts_in, tgt_in, scale_in, mean, whitening, cov, prec, nat, out, nat_out, fit_out,
    zall, pts, tgt, wv, cross, acc, square, pmv, covb,
    wbuf, pay, y1, y2, zs, zr, xk, xs, xr, qay, qx, qs, q1, q2, qz, qr, fin, fint, own, pmr, vec, vy, vz, vx, va, vb, row,
    i_s, i_r, c_s, cov_s, cov_r,
    g_s, g_r, p_s, p_r, y1_s, y1_r, y2_s, y2_r, z_s, z_r, x_s, x_r,
    qx_s, qx_r, q1_s, q1_r, q2_s, q2_r, qz_s, qz_r, dz_s, dz_r, dq_s, pm_s, pm_r, f_s, own_sem, v_s, v_r,
):
    z, lo, y, hi, core = place()
    mine = hi * 2 + core
    yp, ym, y2p = (y + 1) % 4, (y + 3) % 4, (y + 2) % 4
    partner = (z, lo, y, hi, 1 - core)
    gather_to = (z, 1 - lo, y, 1 - hi, (core + 1 - hi) % 2)

    count = pts.shape[1]
    cut = wv.shape[2]
    w_copies = [
        pltpu.make_async_copy(
            whitening.at[:, pl.ds(pl.multiple_of((hi + h - 2 * hi * h) * cut, cut), cut)], wv.at[h], c_s.at[h]
        )
        for h in range(2)
    ]
    for c in w_copies:
        c.start()
    line = [
        (z, (lo + d // 4) % 2, y, (hi + (d // 2) % 2) % 2, (core + d % 2) % 2) for d in range(1, 8)
    ]
    over_y = [(z, lo, (y + d) % 4, hi, core) for d in range(1, 4)]
    over_z = [((z + d) % 8, lo, y, hi, core) for d in range(1, 8)]
    low, high = hi * 2, hi * 2 + 1
    nxt = (1 - hi) * 2 + (core + hi) % 2
    prv = (1 - hi) * 2 + (core + 1 - hi) % 2

    def owner(q, ind):
        return (q // 8, (q // 4) % 2, q % 4, ind // 2, ind % 2)

    def flat(d):
        return (((d[0] * 2 + d[1]) * 4 + d[2]) * 2 + d[3]) * 2 + d[4]

    def equal(a, b):
        return 1 - jnp.minimum(jnp.abs(a - b), 1)

    me = flat(place())
    here = 4 * y + 2 * lo
    holders = (
        [owner(16 * mine + here + e, mine) for e in range(2)]
        + [owner(16 * nxt + here + e, mine) for e in range(2)]
        + [owner(16 * mine + 2 * z + e, nxt) for e in range(2)]
        + [owner(16 * high + here + core, low)]
        + [owner(16 * low + 2 * z + e, high) for e in range(2)]
        + [owner(16 * mine + 2 * z + e, mine) for e in range(2)]
    )

    def ahead(half):
        return (z - 2 * y - half + 8) % 8

    def formed(half):
        return 1 - jnp.minimum(ahead(half) // 5, 1)

    alone = equal(ahead(lo), 0) + jnp.minimum(ahead(lo) // 4, 1)
    needed = [formed(lo)] * 2 + [1] * 7 + [1 - alone] * 2
    own_group, own_q = z // 2, (z % 2) * 8 + lo * 4 + y
    is_d, is_n, is_p = equal(own_group, mine), equal(own_group, nxt), equal(own_group, prv)
    is_s = 1 - is_d - is_n - is_p
    both = is_s * core

    def cov_target(i, second):
        e = own_q % 2
        far = is_d * jnp.minimum((i - own_q // 2 + 8) % 8 // 5, 1)
        mirrored = is_p + is_s * core + far
        to_core = is_p * (own_group % 2) + is_s * ((1 - core) * e + core * second) + (1 - is_p - is_s) * core
        to = (
            (1 - mirrored) * i + mirrored * (own_q // 2),
            (1 - mirrored) * ((own_q // 2) % 2) + mirrored * (i % 2),
            (1 - mirrored) * (own_q // 4) + mirrored * (i // 2),
            is_p * (own_group // 2) + (1 - is_p) * hi,
            to_core,
        )
        slot = is_d * e + far * 9 + is_n * (2 + e) + is_p * (4 + e) + is_s * ((1 - core) * 6 + core * (7 + e))
        return to, cov.at[:, pl.ds(pl.multiple_of(i * 128, 128), 128)], covb.at[slot], cov_r.at[is_d + far]

    covb[...] = jnp.zeros(covb.shape, F32)
    fin[...] = jnp.zeros(fin.shape, BF16)
    barrier = pltpu.get_barrier_semaphore()
    arrivals = 17 + 8 * (1 + both)
    for to in over_y + over_z + line:
        pl.semaphore_signal(barrier, inc=1, device_id=to, device_id_type=MESH)
    for to, need in zip(holders, needed):
        arrivals = arrivals - need * equal(flat(to), me)

        @pl.when(need * (1 - equal(flat(to), me)) == 1)
        def _(to=to):
            pl.semaphore_signal(barrier, inc=1, device_id=to, device_id_type=MESH)

    pl.semaphore_wait(barrier, arrivals)

    over_a = [((z + d) % 8, lo, y, hi, (core + c) % 2) for d in range(8) for c in range(2) if d + c]
    over_b = [
        (z, (lo + a) % 2, (y + d) % 4, (hi + b) % 2, core)
        for d in range(4)
        for a in range(2)
        for b in range(2)
        if d + a + b
    ]

    def cov_sends(second, act):
        def one(i, carry):
            to, src, dst, sem = cov_target(i, second)

            @pl.when(flat(to) != me)
            def _():
                act(remote(src, dst, cov_s.at[8 * second + i], sem, to), True)

            @pl.when(flat(to) == me)
            def _():
                act(pltpu.make_async_copy(src, dst, sem), False)

            return carry

        lax.fori_loop(0, 8, one, 0)

    def cov_start(copy, far):
        copy.start()

    def cov_sent(copy, far):
        if far:
            copy.wait_send()

    def vec_into(k):
        return (vy, vz, vx, va, vb)[k]

    def vec_send(k, src):
        for i, to in enumerate((over_y, over_z, [(z, 1 - lo, y, hi, core)], over_a, over_b)[k]):
            remote(src, vec_into(k).at[i], v_s.at[k], v_r.at[k], to).start()

    def vec_sum(k, src):
        into = vec_into(k)
        remote(into, into, v_s.at[k], v_r.at[k], partner).wait_recv()
        total = src[...]
        return total + sum(into[i] for i in range(into.shape[0]))

    other = (1 - hi) * 2 + core
    across = (z, 1 - lo, y, 1 - hi, core)
    swap = (z, 1 - lo, y, hi, core)
    over = remote(ind_t, zall.at[mine], i_s.at[0], i_r.at[0], across)
    near = remote(ind_t, zall.at[mine], i_s.at[1], i_r.at[1], partner)
    on = remote(zall.at[other], zall.at[other], i_s.at[2], i_r.at[2], partner)
    swaps = (
        remote(pts_in, pts, i_s.at[3], i_r.at[3], swap),
        remote(tgt_in, tgt, i_s.at[4], i_r.at[4], swap),
    )

    @pl.when(hi == 0)
    def _():
        for c in swaps:
            c.start()

    over.start()
    near.start()
    own_z = pltpu.make_async_copy(ind_t, zall.at[mine], c_s.at[2])
    own_z.start()

    @pl.when(hi == 1)
    def _():
        pts[...] = pts_in[...]
        tgt[...] = tgt_in[...]

    own_z.wait()

    @pl.when(hi == 0)
    def _():
        for c in swaps:
            c.wait()

    diagonal = lax.broadcasted_iota(jnp.int32, (64, 64), 0) == lax.broadcasted_iota(jnp.int32, (64, 64), 1)
    scale = jnp.sum(jnp.where(diagonal, jnp.broadcast_to(scale_in[...], (64, 64)), 0.0), axis=1, keepdims=True)
    scales = jnp.broadcast_to(scale, (64, count))
    t_row = jnp.concatenate([tgt[j : j + 1, :] for j in range(count // 128)], axis=1)
    norm_x = 0.5 * jnp.sum(jnp.square(pts[...].astype(F32) / scales), axis=0, keepdims=True)
    three = lax.broadcasted_iota(jnp.int32, (16, count), 0) < 3
    p_mat = jnp.concatenate([pts[...]] * 3 + [jnp.where(three, 1.0, 0.0).astype(BF16)], axis=0)

    def cross_rows(held, half, at):
        def piece(j, carry):
            cols = pl.ds(pl.multiple_of(j * 256, 256), 256)
            zt = zall[held, :, cols]
            s = jnp.broadcast_to(scale, (64, 256))
            zs_ = zt / s
            norm = tile_of(-0.5 * jnp.sum(zs_ * zs_, axis=0, keepdims=True))
            z_mat = jnp.concatenate([*parts_of(zs_ / s), norm], axis=0)
            power = dot(z_mat, p_mat, (0, 0)) - norm_x
            rows = pl.ds(pl.multiple_of(at * 1024 + j * 256, 256), 256)
            cross[half, rows, :] = (hypers[0] * jnp.exp(power)).astype(BF16)
            return carry

        lax.fori_loop(0, 4, piece, 0)

    cross_rows(mine, 0, core)
    near.wait_recv()
    cross_rows(hi * 2 + 1 - core, 0, 1 - core)
    w_copies[0].wait()

    def first_half(i, carry):
        rows = pl.ds(pl.multiple_of(i * 256, 256), 256)
        for j in range(count // 256):
            cols = slice(256 * j, 256 * j + 256)
            acc[rows, cols] = dot(wv[0, rows, :], cross[0, :, cols], (1, 0))
        return carry

    lax.fori_loop(0, 3, first_half, 0)
    over.wait_recv()
    on.start()
    cov_sends(0, cov_start)

    @pl.when(both == 1)
    def _():
        cov_sends(1, cov_start)

    lax.fori_loop(3, 4, first_half, 0)
    cross_rows(other, 1, core)
    on.wait_recv()
    cross_rows((1 - hi) * 2 + 1 - core, 1, 1 - core)
    w_copies[1].wait()
    square[...] = jnp.zeros((8, 128), F32)

    def gather_start(c):
        first, size = PIECES[c]

        def one(k, carry):
            rows = pl.ds(pl.multiple_of(k * 128 + first, 16), size)
            remote(wbuf.at[core, rows], wbuf.at[2, rows], g_s.at[c], g_r.at[c], gather_to).start()
            return carry

        lax.fori_loop(0, 8, one, 0)

    def second_half(g, carry):
        rows = [pl.ds(pl.multiple_of(k * 128 + 32 * g, 32), 32) for k in range(8)]
        a = jnp.concatenate([wv[1, r, :] for r in rows], axis=0)
        for j in range(count // 256):
            cols = slice(256 * j, 256 * j + 256)
            part = dot(a, cross[1, :, cols], (1, 0)) + jnp.concatenate([acc[r, cols] for r in rows], axis=0)
            part = part.astype(BF16)
            for k, r in enumerate(rows):
                wbuf[core, r, cols] = part[32 * k : 32 * k + 32]
            wide = part.astype(F32)
            both = jnp.sum((wide * wide).reshape(32, 8, 256), axis=0)
            square[...] += both[:, :128] + both[:, 128:]
        for c, done in enumerate((0, 2, 3, 3)):

            @pl.when(g == done)
            def _(c=c):
                gather_start(c)

        return carry

    lax.fori_loop(0, 4, second_half, 0)
    to_partner = remote(wbuf.at[core], wbuf.at[core], p_s, p_r, partner)
    to_partner.start()
    def gather_all(g):
        rows = pl.ds(0, 8 * PIECES[g][1])
        return remote(wbuf.at[core, rows], wbuf.at[2, rows], g_s.at[g], g_r.at[g], gather_to)

    up_y, down_y = (z, lo, yp, hi, core), (z, lo, ym, hi, core)
    over_x = (z, 1 - lo, y, hi, core)

    def block(k, size):
        return pl.ds(pl.multiple_of(k * size, size), size)

    def wide(t):
        return pl.ds(0, 640 if t < 2 else 1024)

    def y1_copies(t):
        h, w = TALL[t], wide(t)
        return tuple(
            remote(pay.at[t, block(2 * y2p + k, h), w], y1.at[t, k, pl.ds(0, h), w], y1_s.at[t, k], y1_r.at[t, k], to)
            for k, to in enumerate((up_y, down_y))
        )

    def y2_copies(t):
        h, w = 2 * TALL[t], wide(t)
        return tuple(
            remote(pay.at[t, block(at, h), w], y2.at[t, k, pl.ds(0, h), w], y2_s.at[t, k], y2_r.at[t, k], to)
            for k, (at, to) in enumerate(((yp, up_y), (ym, down_y)))
        )

    def d_copies(t, second):
        halves = (lo,) if second else (0, 1)
        out = []
        for h, half in enumerate(halves):
            for d in range(5):
                to = (2 * y + half + d) % 8
                slot = (to - z + 7) % 8
                cols = slice(128 * d, 128 * d + 128)
                if second:
                    c = (qz.at[t, :, cols], qr.at[t, slot], dq_s.at[t, d], qz_r.at[t])
                else:
                    rows = pl.ds(32 * h, 32)
                    c = (zs.at[t, rows, cols], zr.at[t, slot, rows], dz_s.at[t, 5 * h + d], dz_r.at[t, h])
                out.append((to, c))
        return out

    def d_act(t, second, act):
        for to, c in d_copies(t, second):

            @pl.when(to != z)
            def _(to=to, c=c):
                act(remote(*c, (to, lo, y, hi, core)))

    def z_send(t):
        if t < 2:
            d_act(t, 0, lambda c: c.start())
            return
        for d in range(1, 8):
            to = (z + d) % 8
            rows = pl.ds(0, 2 * TALL[t])
            remote(zs.at[t, rows, block(to, 128)], zr.at[t, d - 1, rows], z_s.at[t], z_r.at[t], over_z[d - 1]).start()

    def z_all(t):
        part = zr.at[t, :, pl.ds(0, 2 * TALL[t])]
        return remote(part, part, z_s.at[t], z_r.at[t], over_x)

    def x_copy(t):
        rows = pl.ds(0, TALL[t])
        return remote(xs.at[t, rows], xr.at[t, rows], x_s.at[t], x_r.at[t], over_x)

    def qx_copy(t):
        return remote(qay.at[t, block(1 - lo, 128), wide(t)], qx.at[t, :, wide(t)], qx_s.at[t], qx_r.at[t], over_x)

    def q1_copies(t):
        return (
            remote(qs.at[t, block(2 * y2p, 16), wide(t)], q1.at[t, 0, :, wide(t)], q1_s.at[t, 0], q1_r.at[t, 0], up_y),
            remote(qs.at[t, block(2 * y2p + 1, 16), wide(t)], q1.at[t, 1, :, wide(t)], q1_s.at[t, 1], q1_r.at[t, 1], down_y),
        )

    def q2_copies(t):
        return (
            remote(qs.at[t, block(yp, 32), wide(t)], q2.at[t, 0, :, wide(t)], q2_s.at[t, 0], q2_r.at[t, 0], up_y),
            remote(qs.at[t, block(ym, 32), wide(t)], q2.at[t, 1, :, wide(t)], q2_s.at[t, 1], q2_r.at[t, 1], down_y),
        )

    def qz_send(t):
        if t < 2:
            d_act(t, 1, lambda c: c.start())
            return
        for d in range(1, 8):
            to = (z + d) % 8
            remote(qz.at[t, :, block(to, 128)], qr.at[t, d - 1], qz_s.at[t], qz_r.at[t], over_z[d - 1]).start()

    def qz_all(t):
        return remote(qr.at[t], qr.at[t], qz_s.at[t], qz_r.at[t], over_x)

    def slab(t, first, h, groups, into):
        is_b, is_h, _ = round_of(t)
        plain = 1 - is_h
        left = is_b * 2 + is_h + plain * (1 - is_b) * core
        right = plain * core
        first = first + is_h * 64 * core
        a = jnp.concatenate([wbuf[left, pl.ds(pl.multiple_of(k * 128 + first, 16), h), :] for k in groups], axis=0)
        for j in range(4):
            b = wbuf[right, j * 256 : (j + 1) * 256, :]
            part = dot(a, b, (1, 1)).astype(BF16)
            if t > 1:
                into[t, : 8 * h, j * 256 : (j + 1) * 256] = part
                continue
            for r, k in enumerate(groups):
                for h in range(2):
                    d = (2 * j + h - k) % 8
                    if d < 5:
                        into[t, 32 * r : 32 * r + 32, 128 * d : 128 * d + 128] = part[
                            32 * r : 32 * r + 32, 128 * h : 128 * h + 128
                        ]

    def qx_start(t):
        is_b, is_h, g = round_of(t)

        if t == 2:
            to_partner.wait_recv()
        if t > 2:
            gather_all(g).wait_recv()
        slab(t, PIECES[g][0] if t > 2 else 32 * g, 32, (0, 2, 4, 6, 1, 3, 5, 7), qay)
        qx_copy(t).start()

    def y1_start(t):
        is_b, is_h, g = round_of(t)

        if t > 2:
            gather_all(g + 1).wait_recv()
        slab(t, PIECES[g + 1][0] if t > 2 else 32 * (g + 1), TALL[t], range(8), pay)
        for c in y1_copies(t):
            c.start()

    def after_qx(t):
        qx_copy(t).wait_recv()
        w = wide(t)
        qs[t, :, w] = (qay[t, block(lo, 128), w].astype(F32) + qx[t, :, w].astype(F32)).astype(BF16)
        for c in q1_copies(t):
            c.start()

    def after_y1(t):
        for k, c in enumerate(y1_copies(t)):
            c.wait_recv()
            h, w = TALL[t], wide(t)
            rows = block(2 * (yp, ym)[k] + k, h)
            pay[t, rows, w] = (pay[t, rows, w].astype(F32) + y1[t, k, :h, w].astype(F32)).astype(BF16)
        for c in y2_copies(t):
            c.start()

    def after_q1(t):
        for k, c in enumerate(q1_copies(t)):
            c.wait_recv()
            rows = block(2 * (yp, ym)[k] + k, 16)
            w = wide(t)
            qs[t, rows, w] = (qs[t, rows, w].astype(F32) + q1[t, k, :, w].astype(F32)).astype(BF16)
        for c in q2_copies(t):
            c.start()

    def after_y2(t):
        for c in y2_copies(t):
            c.wait_recv()
        h, w = 2 * TALL[t], wide(t)
        total = pay[t, block(y, h), w].astype(F32) + y2[t, 0, :h, w].astype(F32) + y2[t, 1, :h, w].astype(F32)
        zs[t, :h, w] = total.astype(BF16)
        z_send(t)

    def after_q2(t):
        for c in q2_copies(t):
            c.wait_recv()
        w = wide(t)
        total = qs[t, block(y, 32), w].astype(F32) + q2[t, 0, :, w].astype(F32) + q2[t, 1, :, w].astype(F32)
        qz[t, :, w] = total.astype(BF16)
        qz_send(t)

    def after_z(t):
        if t < 2:
            for h in range(2):
                rows = pl.ds(32 * h, 32)

                @pl.when(formed(h) == 1)
                def _(h=h, rows=rows):
                    remote(zr.at[t, :, rows], zr.at[t, :, rows], x_s.at[t], dz_r.at[t, h], over_x).wait_recv()
                    total = zs[t, rows, block(jnp.minimum(ahead(h), 4), 128)].astype(F32)
                    xk[t, rows, :] = total + sum(zr[t, d, rows].astype(F32) for d in range(7))

            @pl.when(formed(1 - lo) == 1)
            def _():
                xs[t, :32] = xk[t, block(1 - lo, 32), :].astype(BF16)
                x_copy(t).start()

            return
        z_all(t).wait_recv()
        h = TALL[t]
        total = zs[t, : 2 * h, block(z, 128)].astype(F32)
        for d in range(7):
            total = total + zr[t, d, : 2 * h].astype(F32)
        xk[t, : 2 * h] = total
        xs[t, :h] = xk[t, block(1 - lo, h), :].astype(BF16)
        x_copy(t).start()

    def finish(t, second, total):
        is_b, is_h, g = round_of(t)
        first = PIECES[g + second][0] if t > 2 else 32 * (g + second)
        rows = pl.ds(pl.multiple_of(first + is_h * core * 64, 16), total.shape[0])
        fin[is_b + 2 * is_h, rows, :] = total.astype(BF16)

    def after_qz(t):
        if t < 2:

            @pl.when(formed(lo) == 1)
            def _():
                qz_all(t).wait_recv()
                total = qz[t, :, block(jnp.minimum(ahead(lo), 4), 128)].astype(F32)
                finish(t, 0, total + sum(qr[t, d].astype(F32) for d in range(7)))

            return
        qz_all(t).wait_recv()
        total = qz[t, :, block(z, 128)].astype(F32)
        for d in range(7):
            total = total + qr[t, d].astype(F32)
        finish(t, 0, total)

    def after_x(t):
        def add():
            x_copy(t).wait_recv()
            h = TALL[t]
            finish(t, 1, xk[t, block(lo, h), :] + xr[t, :h].astype(F32))

        if t < 2:
            pl.when(formed(lo) == 1)(add)
        else:
            add()

    pm_to = (partner, (z, 1 - lo, y, 1 - hi, core), (z, 1 - lo, y, 1 - hi, 1 - core))
    pm_copies = [remote(pmv, pmr.at[k], pm_s.at[k], pm_r.at[k], to) for k, to in enumerate(pm_to)]

    def means_and_proj():
        m_row = jnp.concatenate([mean[j : j + 1, :] for j in range(8)], axis=1)
        pmv[...] = jnp.sum(dot(tile_of(m_row), wbuf[core], (1, 0)), axis=0, keepdims=True)
        for c in pm_copies:
            c.start()
        proj = jnp.sum(dot(tile_of(t_row), wbuf[core], (1, 1)), axis=0, keepdims=True)
        vec[2] = jnp.concatenate([proj[:, 128 * j : 128 * j + 128] for j in range(8)], axis=0)
        vec_send(0, vec.at[2])

    direct = block(z, 128)
    mirror = block(2 * y + lo, 128)
    half = block(core, 64)
    pieces = [fin.at[0, pl.ds(64 * e, 64)] for e in range(2)] + [fin.at[1, pl.ds(64 * e, 64)] for e in range(2)]
    pieces += [fint.at[0, pl.ds(64 * e, 64)] for e in range(2)]
    pieces += [fin.at[2, half]] + [fint.at[1, pl.ds(64 * e, 64)] for e in range(2)]
    pieces += [fint.at[2, pl.ds(64 * e, 64)] for e in range(2)]
    places = [own.at[0, :, direct]] * 4 + [own.at[0, :, mirror]] * 2 + [own.at[0, :, direct]] + [own.at[core, :, mirror]] * 2
    places += [own.at[0, :, mirror]] * 2
    sems = [own_sem.at[0]] * 7 + [own_sem.at[core]] * 2 + [own_sem.at[0]] * 2
    sends = list(zip(pieces, places, sems, holders))

    def deliver(some):
        for k in some:
            src, dst, sem, to = sends[k]

            @pl.when(needed[k] * (1 - equal(flat(to), me)) == 1)
            def _(k=k, src=src, dst=dst, sem=sem, to=to):
                remote(src, dst, f_s.at[k], sem, to).start()

            @pl.when(needed[k] * equal(flat(to), me) == 1)
            def _(src=src, dst=dst, sem=sem):
                pltpu.make_async_copy(src, dst, sem).start()

        return sum(
            jnp.sum((covb[k] * pieces[k][...].astype(F32)).reshape(8, 8, 128), axis=0) for k in some
        )

    def early():
        for c in pm_copies:
            c.wait_recv()
        resid = t_row - (pmv[...] + pmr[0] + pmr[1] + pmr[2])
        resid = resid * resid
        total = sum(resid[:, 128 * j : 128 * j + 128] for j in range(count // 128))
        total = jnp.broadcast_to(total / 32, (8, 128)) - square[...]
        fint[1] = fin[2].astype(F32).T.astype(BF16)
        fint[2] = fin[0].astype(F32).T.astype(BF16)
        for k, first, last in ((0, 2, 9), (1, 0, 2), (2, 9, 11)):
            some = covb.at[pl.ds(first, last - first)]

            @pl.when(needed[first] == 1)
            def _(k=k, some=some):
                pltpu.make_async_copy(some, some, cov_r.at[k]).wait()

        return total + deliver((0, 1, 6, 7, 8, 9, 10))

    order = (
        (qx_start, 0), (y1_start, 0), (qx_start, 1), (y1_start, 1), (qx_start, 2), (y1_start, 2), (qx_start, 3),
        (after_qx, 0), (after_y1, 0), (after_y1, 1), (after_y1, 2), (after_q1, 0), (after_qx, 1), (after_y2, 0),
        (after_y2, 1), (after_qx, 2), (after_y2, 2), (after_q2, 0), (after_q1, 1), (y1_start, 3), (after_z, 0),
        (after_q1, 2), (after_z, 1), (after_q2, 1), (after_qx, 3), (after_x, 0), (after_x, 1), (after_y1, 3),
        (after_z, 2), (after_q2, 2), (after_qz, 0), (after_q1, 3), (after_qz, 1), (qx_start, 4), (after_x, 2),
        (after_y2, 3), (after_qz, 2), (y1_start, 4), (after_q2, 3), (after_y1, 4), (after_qx, 4), (after_y2, 4),
        (after_q1, 4), (after_z, 3), (after_qz, 3), (after_x, 3), (after_q2, 4), (after_z, 4), (after_x, 4),
        (after_qz, 4),
    )
    for at, (work, t) in enumerate(order):
        if at == 4:
            means_and_proj()
        if at == 12:
            vec[0] = vec_sum(0, vec.at[2])
            vec_send(1, vec.at[0])
        if at == 24:
            vec[1] = vec_sum(1, vec.at[0])
            vec_send(2, vec.at[1])
        work(t)
        if at == 36:
            partial = early()

    fint[0] = fin[1].astype(F32).T.astype(BF16)
    total = partial + deliver((2, 3, 4, 5))
    row[0] = jnp.sum(total, axis=0, keepdims=True)
    vec_send(3, row.at[0])
    per_noise = 0.5 / hypers[1]
    nat_out[...] = 0.5 * nat[...] + vec_sum(2, vec.at[1]) * per_noise
    row[1] = vec_sum(3, row.at[0])
    vec_send(4, row.at[1])

    pltpu.make_async_copy(own.at[0], own.at[0], own_sem.at[0]).wait()

    @pl.when(both == 1)
    def _():
        pltpu.make_async_copy(own.at[1], own.at[1], own_sem.at[1]).wait()
        own[0] = own[0] + own[1]

    gap = ((z * 2 + lo) * 4 + y) * 64 - mine * 1024
    for i in range(8):
        rows = slice(8 * i, 8 * i + 8)
        shape = (8, 1024)
        same = lax.broadcasted_iota(jnp.int32, shape, 1) - lax.broadcasted_iota(jnp.int32, shape, 0) == gap + 8 * i
        out[rows] = 0.5 * prec[rows] + (jnp.where(same, 0.5, 0.0) + own[0, rows].astype(F32) * per_noise)

    points = 64.0 * count
    total = jnp.sum(vec_sum(4, row.at[1]), axis=(0, 1), keepdims=True) + hypers[0] * points
    noise = jnp.full((1, 1), hypers[1], F32)
    fit_out[...] = -0.5 * jnp.log(2.0 * jnp.pi * noise) - total / (2.0 * noise * points)
    for k in range(5):
        into = vec_into(k)
        remote(into, into, v_s.at[k], v_r.at[k], partner).wait_send()
    cov_sends(0, cov_sent)

    @pl.when(both == 1)
    def _():
        cov_sends(1, cov_sent)

    for k, (src, dst, sem, to) in enumerate(sends):

        @pl.when(needed[k] * (1 - equal(flat(to), me)) == 1)
        def _(k=k, src=src, dst=dst, sem=sem, to=to):
            remote(src, dst, f_s.at[k], sem, to).wait_send()

    for c in pm_copies:
        c.wait_send()
    for c in (over, near, on, to_partner):
        c.wait_send()

    for t in range(ROUNDS):
        for c in y1_copies(t) + y2_copies(t) + q1_copies(t) + q2_copies(t) + (qx_copy(t),):
            c.wait_send()
        if t < 2:
            d_act(t, 0, lambda c: c.wait_send())
            d_act(t, 1, lambda c: c.wait_send())
            pl.when(formed(1 - lo) == 1)(x_copy(t).wait_send)
        else:
            for c in (z_all(t), x_copy(t), qz_all(t)):
                c.wait_send()
    for c in range(4):
        gather_all(c).wait_send()


def step(hypers, ind_t, pts, tgt, scale, mean, whitening, cov, prec, nat):
    dma = pltpu.SemaphoreType.DMA
    n = pts.shape[1]
    return pl.pallas_call(
        kernel,
        out_shape=tuple(jax.ShapeDtypeStruct(s, F32) for s in ((64, 1024), (8, 128), (1, 1))),
        in_specs=[pl.BlockSpec(memory_space=pltpu.SMEM)] + [VMEM] * 5 + [ANY] + [VMEM] * 3,
        out_specs=(VMEM, VMEM, VMEM),
        scratch_shapes=[
            pltpu.VMEM((4, 64, 1024), F32),
            pltpu.VMEM((64, n), BF16),
            pltpu.VMEM(tgt.shape, F32),
            pltpu.VMEM((2, 1024, 2048), BF16),
            pltpu.VMEM((2, 2048, n), BF16),
            pltpu.VMEM((1024, n), F32),
            pltpu.VMEM((8, 128), F32),
            pltpu.VMEM((1, n), F32),
            pltpu.VMEM((11, 64, 128), F32),
            pltpu.VMEM((3, 1024, n), BF16),
            pltpu.VMEM((ROUNDS, 8 * max(TALL), 1024), BF16),
            pltpu.VMEM((ROUNDS, 2, max(TALL), 1024), BF16),
            pltpu.VMEM((ROUNDS, 2, 2 * max(TALL), 1024), BF16),
            pltpu.VMEM((ROUNDS, 2 * max(TALL), 1024), BF16),
            pltpu.VMEM((ROUNDS, 7, 2 * max(TALL), 128), BF16),
            pltpu.VMEM((ROUNDS, 2 * max(TALL), 128), F32),
            pltpu.VMEM((ROUNDS, max(TALL), 128), BF16),
            pltpu.VMEM((ROUNDS, max(TALL), 128), BF16),
            pltpu.VMEM((ROUNDS, 256, 1024), BF16),
            pltpu.VMEM((ROUNDS, 128, 1024), BF16),
            pltpu.VMEM((ROUNDS, 128, 1024), BF16),
            pltpu.VMEM((ROUNDS, 2, 16, 1024), BF16),
            pltpu.VMEM((ROUNDS, 2, 32, 1024), BF16),
            pltpu.VMEM((ROUNDS, 32, 1024), BF16),
            pltpu.VMEM((ROUNDS, 7, 32, 128), BF16),
            pltpu.VMEM((3, 128, 128), BF16),
            pltpu.VMEM((3, 128, 128), BF16),
            pltpu.VMEM((2, 64, 1024), BF16),
            pltpu.VMEM((3, 1, n), F32),
            pltpu.VMEM((3, 8, 128), F32),
            pltpu.VMEM((3, 8, 128), F32),
            pltpu.VMEM((7, 8, 128), F32),
            pltpu.VMEM((1, 8, 128), F32),
            pltpu.VMEM((15, 1, 128), F32),
            pltpu.VMEM((15, 1, 128), F32),
            pltpu.VMEM((2, 1, 128), F32),
            dma((5,)), dma((5,)), dma((3,)), dma((16,)), dma((3,)),
            dma((4,)), dma((4,)), dma, dma,
            dma((ROUNDS, 2)), dma((ROUNDS, 2)), dma((ROUNDS, 2)), dma((ROUNDS, 2)),
            dma((ROUNDS,)), dma((ROUNDS,)), dma((ROUNDS,)), dma((ROUNDS,)),
            dma((ROUNDS,)), dma((ROUNDS,)), dma((ROUNDS, 2)), dma((ROUNDS, 2)),
            dma((ROUNDS, 2)), dma((ROUNDS, 2)), dma((ROUNDS,)), dma((ROUNDS,)),
            dma((2, 10)), dma((2, 2)), dma((2, 5)),
            dma((3,)), dma((3,)), dma((11,)), dma((2,)), dma((5,)), dma((5,)),
        ],
        compiler_params=pltpu.CompilerParams(has_side_effects=True, collective_id=0, vmem_limit_bytes=56 * 2**20),
        name="gp_step",
    )(hypers, ind_t, pts, tgt, scale, mean, whitening, cov, prec, nat)


def shards(points, targets, inducing, whitening, mean_v, covariance, precision, natural_one, lengthscales, hypers):
    own_rows, own_points = inducing.shape[0], points.shape[0]
    precision_new, natural_new, expected_fit = step(
        hypers,
        inducing.T,
        points.T,
        targets.reshape(own_points // 128, 128),
        lengthscales.reshape(1, -1),
        mean_v.reshape(8, 128),
        whitening,
        covariance.T,
        precision.T,
        natural_one.reshape(8, 128),
    )
    return precision_new.T, natural_new.reshape(own_rows), expected_fit.reshape(())


def solution(mesh):
    finer = Mesh(mesh.devices.reshape(8, 2, mesh.shape["rep"], 2, 2), AXES)
    return jax.shard_map(
        shards,
        mesh=finer,
        in_specs=(
            P(DP_REP, None), P(DP_REP), P(IND, None), P(IND, None), P(IND),
            P(IND, DP_REP), P(IND, DP_REP), P(IND), P(), P(),
        ),
        out_specs=(P(IND, DP_REP), P(IND), P()),
        check_vma=False,
    )
```
